256 devices in a mesh: trait: 4 (over x, y), ppl: 64 (over z, core).
Axes of the slice: x: 2, y: 2, z: 32, core: 2. Of those that a mesh axis runs over, the one named last changes fastest.
The devices are a block of a 4x8x32 slice.
Arguments:
- genotypes: bfloat16 [65536, 4096], P(('trait', 'ppl')), parts along dimension 0
- residual: float32 [128, 16384], P('trait', 'ppl'), parts along dimension 0, may hold values from -36 to 36
- noise_people: float32 [128, 16384], P('trait', 'ppl'), parts along dimension 0, may hold values from -6 to 6
- noise_coef: float32 [128, 4096], P('trait'), parts along dimension 0, may hold values from -6 to 6
- coef_all: float32 [128, 8192], P('trait'), parts along dimension 0, may hold values from -0.06 to 0.06
- block_index: int32 [4], P('trait'), parts along dimension 0, may hold values from 0 to 1
- prior_prec: float32 [128], P('trait'), parts along dimension 0, may hold values from 82 to 410
- sigma2_old: float32 [128], P('trait'), parts along dimension 0, may hold values from 0.5 to 2
- gamma_draw: float32 [128], P('trait'), parts along dimension 0, may hold values from 0.8 to 1.25
- valid_counts: int32 [256], P('trait'), parts along dimension 0, may hold values from 128 to 256, as said below
Outputs:
- coef_new: float32 [128, 8192], P('trait'), parts along dimension 0
- residual_new: float32 [128, 16384], P('trait', 'ppl'), parts along dimension 0
- sigma2_new: float32 [128], P('trait'), parts along dimension 0
The draws below stay inside these ranges and needn't reach their ends.
There are 4 independent parts, one for each index of `trait`. The reference program is written for one: setup_inputs(seed, part) draws one part's arguments, and reference() takes and returns one part's arrays. A program takes and returns all parts, laid end to end along the dimension named above; each array names one. Nothing has to cross between parts.
Inputs may be any that keep to these rules, and one draw needn't show every extreme that they name: `valid_counts`: each entry counts the people present in one device's 256 slots; they fill the lowest slots, and some entry equals 256.
All inputs are finite; a program needn't handle non-finite values.
Results may differ from the reference program's by a relative error of at most 0.0049.
Values may be sent and summed in bfloat16 or wider, within the bound.
A program may use at most 64 MiB of HBM per device.

```python
import math
import jax
import jax.numpy as jnp
from jax import lax

ROWS_DEV = 256
BATCH = 4096
TRAITS = 32
ITERS = 4
BLOCKS = 2
PEOPLE = 16384
VARS = 8192
N_PPL = 64


def draw_genotypes(key, part):
    inner_key = jax.random.fold_in(key, 11)
    innov = jax.random.normal(inner_key, (PEOPLE, BATCH + 2), jnp.float32)
    blended = innov[:, 1:-1] + 0.45 * (innov[:, :-2] + innov[:, 2:])
    return (blended / jnp.sqrt(1.405)).astype(jnp.bfloat16)


def draw_residual(key, part):
    inner_key = jax.random.fold_in(key, 23)
    position = jnp.arange(PEOPLE, dtype=jnp.float32) / PEOPLE
    base = jax.random.normal(inner_key, (TRAITS, PEOPLE), jnp.float32)
    scale_line = 1.0 + 2.0 * position
    return jnp.clip(base, -6.0, 6.0) * scale_line[None, :]


def draw_valid_counts(key, part):
    inner_key = jax.random.fold_in(key, 7)
    key_counts, key_full = jax.random.split(inner_key)
    drawn_counts = jax.random.randint(key_counts, (N_PPL,), ROWS_DEV // 2, ROWS_DEV + 1)
    full_shard = jax.random.randint(key_full, (), 0, N_PPL)
    filled = jnp.where(jnp.arange(N_PPL) == full_shard, ROWS_DEV, drawn_counts)
    return filled.astype(jnp.int32)


def levels(rng, dims, cuts, low, high):
    factor_of, own = 1.0, jax.random.fold_in(rng, 6)
    for dim, blocks in cuts:
        steps = jnp.exp(jax.random.uniform(jax.random.fold_in(own, dim), (blocks,), jnp.float32, low / len(cuts), high / len(cuts)))
        factor_of = factor_of * jnp.repeat(steps, dims[dim] // blocks).reshape([-1 if axis == dim else 1 for axis in range(len(dims))])
    return factor_of


def normal_values(stream_key, extent, scale, limit, shards=(), kind=jnp.bfloat16):
    loudness = levels(stream_key, extent, shards, -0.22, 0.18) if shards else 1.0
    entries = jax.random.normal(stream_key, extent, jnp.float32) * scale * loudness
    return jnp.minimum(jnp.maximum(entries, -limit), limit).astype(kind)


def setup_inputs(seed: int = 0, part: int = 0) -> dict:
    seeds = jax.random.split(jax.random.key(seed), 11)
    own_keys = jax.random.split(jax.random.fold_in(seeds[10], part), 11)
    return {
        "genotypes": draw_genotypes(jax.random.fold_in(jax.random.fold_in(seeds[10], part), 71), part),
        "residual": draw_residual(jax.random.fold_in(jax.random.fold_in(seeds[10], part), 71), part),
        "noise_people": normal_values(own_keys[2], (TRAITS, PEOPLE), 1.0, 6.0, ((1, 64),), jnp.float32),
        "noise_coef": normal_values(own_keys[3], (TRAITS, BATCH), 1.0, 6.0, (), jnp.float32),
        "coef_all": normal_values(own_keys[4], (TRAITS, VARS), 0.01, 0.06, (), jnp.float32),
        "block_index": jax.random.randint(own_keys[5], (1,), 0, BLOCKS).astype(jnp.int32),
        "prior_prec": jnp.clip(jnp.exp(jax.random.uniform(own_keys[6], (TRAITS,), jnp.float32, math.log(82.0), math.log(410.0))), 82.0, 410.0),
        "sigma2_old": jnp.clip(jnp.exp(jax.random.uniform(own_keys[7], (TRAITS,), jnp.float32, math.log(0.5), math.log(2.0))), 0.5, 2.0),
        "gamma_draw": jnp.clip(jax.random.uniform(own_keys[8], (TRAITS,), jnp.float32, 0.8, 1.25), 0.8, 1.25),
        "valid_counts": draw_valid_counts(jax.random.fold_in(jax.random.fold_in(seeds[10], part), 71), part),
    }


PRIOR_DOF = 4.0
PRIOR_SCALE = 0.5

def reference(genotypes, residual, noise_people, noise_coef, coef_all, block_index, prior_prec, sigma2_old, gamma_draw, valid_counts):
    people_total = genotypes.shape[0]
    slot_ids = jnp.arange(people_total, dtype=jnp.int32)
    shard_ids = slot_ids // ROWS_DEV
    within = slot_ids % ROWS_DEV
    person_mask = (within < valid_counts[shard_ids]).astype(jnp.float32)[None, :]
    first_col = (block_index[0] * BATCH).astype(jnp.int32)
    old_coef = lax.dynamic_slice_in_dim(coef_all, first_col, BATCH, 1)
    contract = (((1,), (1,)), ((), ()))
    fitted_old = lax.dot_general(old_coef.astype(jnp.bfloat16), genotypes, contract, preferred_element_type=jnp.float32)
    partial_res = person_mask * (residual + fitted_old)
    noise_var = sigma2_old[:, None]
    ridge = prior_prec[:, None]
    target = (person_mask * (partial_res + jnp.sqrt(noise_var) * noise_people)).astype(jnp.bfloat16)
    rhs = jnp.dot(target, genotypes, preferred_element_type=jnp.float32) / noise_var + jnp.sqrt(ridge) * noise_coef
    batch_coef = jnp.zeros_like(rhs)
    fitted = jnp.zeros_like(partial_res)
    search = rhs
    direction = rhs
    norm_now = lax.optimization_barrier(jnp.sum(search * search, axis=1))
    for number in range(ITERS):
        dir_low = direction.astype(jnp.bfloat16)
        dir_full = lax.optimization_barrier(dir_low).astype(jnp.float32)
        image = person_mask * lax.dot_general(dir_low, genotypes, contract, preferred_element_type=jnp.float32)
        image_low = image.astype(jnp.bfloat16)
        applied = jnp.dot(image_low, genotypes, preferred_element_type=jnp.float32) / noise_var + ridge * dir_full
        step_size = norm_now / lax.optimization_barrier(jnp.sum(dir_full * applied, axis=1))
        batch_coef = batch_coef + step_size[:, None] * dir_full
        fitted = fitted + step_size[:, None] * image
        search = search - step_size[:, None] * applied
        norm_next = lax.optimization_barrier(jnp.sum(search * search, axis=1))
        direction = search + (norm_next / norm_now)[:, None] * direction
        norm_now = norm_next
    residual_new = partial_res - fitted
    squares = lax.optimization_barrier(jnp.sum(residual_new * residual_new, axis=1))
    present = jnp.sum(valid_counts).astype(jnp.float32)
    sigma2_new = (squares + PRIOR_DOF * PRIOR_SCALE) / ((present + PRIOR_DOF) * gamma_draw)
    coef_new = lax.dynamic_update_slice_in_dim(coef_all, batch_coef, first_col, 1)
    return (coef_new, residual_new, sigma2_new)
```

```python
import functools

import jax
import jax.numpy as jnp
from jax import lax
from jax.experimental import pallas as pl
from jax.experimental.pallas import tpu as pltpu
from jax.sharding import PartitionSpec as P

ITERS = 4
PRIOR_DOF = 4.0
PRIOR_SCALE = 0.5
AXIS = "ppl"
CORES = 2
NEAR = 8
MESH = pl.DeviceIdType.MESH
F32 = jnp.float32
BF16 = jnp.bfloat16
NT = (((1,), (1,)), ((), ()))
NN = (((1,), (0,)), ((), ()))
CODES = 32000.0
FULL = (3, -3, 2, -2, 1, -1)
ENDS = (NEAR // 2, -(NEAR // 2))
SENDS = ((NEAR // 2, 3, -3), (2, -2), (1, -1), (0,))
TAKES = ((0, 1, -1), (2, -2), (3, -3, NEAR // 2))
SPLIT = True


def kernel(
    chips,
    geno,
    resid,
    npeople,
    ncoef,
    coef,
    block,
    prior,
    sigma,
    gamma,
    counts,
    coef_out,
    resid_out,
    sigma_out,
    xh,
    xo,
    cf,
    res,
    npl,
    nco,
    s_block,
    s_prior,
    s_sigma,
    s_gamma,
    s_counts,
    pres,
    dsend,
    drecv,
    rs_own,
    rs_send,
    rs_recv,
    cv_send,
    cv_recv,
    mid,
    mcv,
    ag,
    agn,
    agn_send,
    search_ref,
    dir_ref,
    dirb_ref,
    acc,
    img_send,
    img_recv,
    dd_send,
    dd_recv,
    img,
    fitted,
    fin,
    c_recv,
    d_recv,
    vals,
    load_sem,
    small_sem,
    pair_send,
    pair_recv,
    st_send,
    st_recv,
):
    traits, rows = res.shape
    width = xo.shape[2]
    half = NEAR * width
    groups = chips // NEAR
    top = traits // 2
    me = lax.axis_index(AXIS)
    z = me // CORES
    k = lax.rem(me, CORES)
    g = z // NEAR
    r = lax.rem(z, NEAR)
    partner = {AXIS: z * CORES + (1 - k)}

    def chip(offset, core):
        return {AXIS: lax.rem(z + offset + chips, chips) * CORES + core}

    def piece_at(offset):
        return lax.rem(r + offset + NEAR, NEAR)

    barrier = pltpu.get_barrier_semaphore()
    greeted = 0
    hello = (NEAR, -NEAR, *ENDS, *FULL) if SPLIT else range(1, chips)
    for offset in hello:
        pl.semaphore_signal(barrier, inc=1, device_id=chip(offset, k), device_id_type=MESH)
        greeted += 1
    for offset in (*FULL, *ENDS, 0):
        pl.semaphore_signal(barrier, inc=1, device_id=chip(offset, 1 - k), device_id_type=MESH)
        greeted += 1

    mine = pl.multiple_of(k * half, half)
    other = pl.multiple_of((1 - k) * half, half)
    own_col = pl.multiple_of(k * half + r * width, width)
    loads = [
        pltpu.make_async_copy(coef.at[:, pl.ds(mine, half)], cf.at[0], load_sem.at[0]),
        pltpu.make_async_copy(coef.at[:, pl.ds(other, half)], cf.at[1], load_sem.at[1]),
        pltpu.make_async_copy(coef.at[:, pl.ds(2 * half + mine, half)], cf.at[2], load_sem.at[2]),
        pltpu.make_async_copy(coef.at[:, pl.ds(2 * half + other, half)], cf.at[3], load_sem.at[3]),
        pltpu.make_async_copy(resid, res, load_sem.at[4]),
        pltpu.make_async_copy(npeople, npl, load_sem.at[5]),
        pltpu.make_async_copy(ncoef.at[:, pl.ds(own_col, width)], nco, load_sem.at[6]),
    ]
    for piece in range(NEAR):
        at = pl.multiple_of(mine + piece * width, width)
        loads.append(
            pltpu.make_async_copy(geno.at[:, pl.ds(at, width)], xh.at[0, piece], load_sem.at[7 + piece])
        )
    for piece in range(NEAR):
        at = pl.multiple_of(other + piece * width, width)
        loads.append(
            pltpu.make_async_copy(geno.at[:, pl.ds(at, width)], xo.at[piece], load_sem.at[15 + piece])
        )
    smalls = [
        pltpu.make_async_copy(block, s_block, small_sem.at[0]),
        pltpu.make_async_copy(prior, s_prior, small_sem.at[1]),
        pltpu.make_async_copy(sigma, s_sigma, small_sem.at[2]),
        pltpu.make_async_copy(gamma, s_gamma, small_sem.at[3]),
        pltpu.make_async_copy(counts, s_counts, small_sem.at[4]),
    ]
    for copy in smalls + loads:
        copy.start()
    for copy in smalls:
        copy.wait()

    row_id = lax.broadcasted_iota(jnp.int32, (traits, 128), 0)
    lane_id = lax.broadcasted_iota(jnp.int32, (traits, 128), 1)

    def to_row(columns):
        total = jnp.zeros((traits, 128), F32)
        for place, column in enumerate(columns):
            total += jnp.where(lane_id == row_id + place * traits, column, 0.0)
        return jnp.sum(total, axis=0, keepdims=True)

    def to_column(line, place):
        return jnp.sum(
            jnp.where(lane_id == row_id + place * traits, line, 0.0), axis=1, keepdims=True
        )

    def column_of(ref):
        column = jnp.zeros((traits, 128), F32)
        for trait in range(traits):
            column = jnp.where(row_id == trait, ref[trait], column)
        return column

    vals[0] = column_of(s_sigma)
    vals[1] = column_of(s_prior)
    vals[2] = column_of(s_gamma)
    noise_var = vals[0][:, 0:1]
    ridge = vals[1][:, 0:1]
    slot = lax.broadcasted_iota(jnp.int32, (traits, rows), 1)
    mask_own = (slot < s_counts[me]).astype(F32)
    mask_pair = (slot < s_counts[z * CORES + (1 - k)]).astype(F32)

    def coded(values):
        largest = jnp.maximum(jnp.max(jnp.abs(values), axis=1, keepdims=True), 1e-30)
        codes = jnp.round(values * (CODES / largest)).astype(jnp.int32).astype(jnp.int16)
        return codes, largest * (1.0 / CODES)

    def decoded(codes, unit):
        return codes.astype(jnp.int32).astype(F32) * unit

    for copy in loads:
        copy.wait()
    first = s_block[0] == 0
    old_mine = jnp.where(first, cf[0], cf[2]).astype(BF16)
    old_other = jnp.where(first, cf[1], cf[3]).astype(BF16)
    fitted_old = jnp.zeros((traits, rows), F32)
    for piece in range(NEAR):
        columns = slice(piece * width, (piece + 1) * width)
        fitted_old += lax.dot_general(old_mine[:, columns], xh[0, piece], NT, preferred_element_type=F32)
        fitted_old += lax.dot_general(old_other[:, columns], xo[piece], NT, preferred_element_type=F32)
    partial_res = mask_own * (res[...] + fitted_old)
    pres[0] = partial_res
    target = (mask_own * (partial_res + jnp.sqrt(noise_var) * npl[...])).astype(BF16)
    for piece in range(NEAR):
        dsend[piece] = lax.dot_general(target, xo[piece], NN, preferred_element_type=F32)
    for piece in range(NEAR):
        dir_ref[piece] = lax.dot_general(target, xh[0, piece], NN, preferred_element_type=F32)
    fitted[...] = jnp.zeros_like(fitted)
    acc[...] = jnp.zeros_like(acc)

    pl.semaphore_wait(barrier, greeted)

    def to_pair(src, dst, index):
        return pltpu.make_async_remote_copy(
            src_ref=src,
            dst_ref=dst,
            send_sem=pair_send.at[index],
            recv_sem=pair_recv.at[index],
            device_id=partner,
            device_id_type=MESH,
        )

    swap_sum = to_pair(dsend, drecv, 0)
    swap_res = to_pair(pres.at[0], pres.at[1], 1)
    swap_geno = to_pair(xo, xh.at[1], 2)
    swap_sum.start()
    swap_res.start()
    swap_geno.start()
    swap_sum.wait_recv()

    def send(src, dst, stage, number, target):
        pltpu.make_async_remote_copy(
            src_ref=src,
            dst_ref=dst,
            send_sem=st_send.at[number, stage],
            recv_sem=st_recv.at[number, stage],
            device_id=target,
            device_id_type=MESH,
        ).start()

    def arrived(ref, stage, number):
        pltpu.make_async_copy(ref, ref, st_recv.at[number, stage]).wait()

    def sum_for_owner(number, part_of, column, relay):
        for offsets in SENDS:
            pieces = [piece_at(offset) for offset in offsets]
            for offset, piece, part in zip(offsets, pieces, [part_of(piece) for piece in pieces]):
                if offset == 0:
                    rs_own[...] = part
                    continue
                rs_send[number, piece], unit = coded(part)
                cv_send[number, piece] = to_row([column, unit])
            for offset, piece in zip(offsets, pieces):
                line = cv_send.at[number, piece]
                codes = rs_send.at[number, piece]
                if offset == ENDS[0]:
                    for place, end in enumerate(ENDS):
                        band = pl.ds(place * top, top)
                        send(line, cv_recv.at[number, 6 + place], 1, number, chip(end, k))
                        send(
                            codes.at[band], rs_recv.at[number, 6, band], 0, number, chip(end, k)
                        )
                elif offset:
                    slot_id = FULL.index(offset)
                    send(line, cv_recv.at[number, slot_id], 1, number, chip(offset, k))
                    send(codes, rs_recv.at[number, slot_id], 0, number, chip(offset, k))
        arrived(cv_recv.at[number], 1, number)
        sums = to_row([column])
        for slot_id in range(7):
            sums += cv_recv[number, slot_id]
        sums = to_column(sums, 0)
        upper = lax.broadcasted_iota(jnp.int32, (traits, 1), 0) < top
        arrived(rs_recv.at[number], 0, number)
        total = rs_own[...]
        for slot_id in range(6):
            total += decoded(rs_recv[number, slot_id], to_column(cv_recv[number, slot_id], 1))
        unit = jnp.where(upper, to_column(cv_recv[number, 6], 1), to_column(cv_recv[number, 7], 1))
        total += decoded(rs_recv[number, 6], unit)
        mid[number, g], unit = coded(total)
        mcv[number, g] = to_row([sums, unit])

        def pass_on(group, offset, stage):
            send(mcv.at[number, group], mcv.at[number, group], stage + 1, number, chip(offset, k))
            send(mid.at[number, group], mid.at[number, group], stage, number, chip(offset, k))

        if not relay:
            pass_on(g, 2 * NEAR, 10)
        pass_on(g, NEAR, 2)
        pass_on(g, -NEAR, 8)
        arrived(mcv.at[number, 0], 9, number)
        arrived(mid.at[number, 0], 8, number)
        if relay:
            pass_on(lax.rem(g + 1, groups), -NEAR, 10)
        arrived(mcv.at[number, 0], 3, number)
        arrived(mid.at[number, 0], 2, number)
        arrived(mcv.at[number, 0], 11, number)
        arrived(mid.at[number, 0], 10, number)
        sums = mcv[number, 0]
        total = decoded(mid[number, 0], to_column(sums, 1))
        for group in range(1, groups):
            line = mcv[number, group]
            sums += line
            total += decoded(mid[number, group], to_column(line, 1))
        return total, to_column(sums, 0)

    def share(number, search, step):
        ag[number, r] = search.astype(BF16)
        agn_send[number] = to_row([jnp.sum(search * search, axis=1, keepdims=True), step])
        line = k * NEAR + r
        agn[number, line] = agn_send[number]
        for offset in (ENDS[0], *FULL):
            send(agn_send.at[number], agn.at[number, line], 5, number, chip(offset, k))
        for offset in (ENDS[0], *FULL, 0):
            send(agn_send.at[number], agn.at[number, line], 5, number, chip(offset, 1 - k))
        for place, end in enumerate(ENDS):
            band = pl.ds(place * top, top)
            send(ag.at[number, r, band], ag.at[number, r, band], 14, number, chip(end, k))
        for offset in FULL:
            send(ag.at[number, r], ag.at[number, r], 11 + abs(offset), number, chip(offset, k))
        arrived(agn.at[number, pl.ds(0, CORES * NEAR - 1)], 5, number)
        line = agn[number, 0]
        for place in range(1, CORES * NEAR):
            line += agn[number, place]
        return to_column(line, 0), to_column(agn[number, 0], 1)

    def image_of(number, ratio):
        squares = jnp.zeros((traits, 1), F32)
        own = jnp.zeros((traits, rows), F32)
        pair = jnp.zeros((traits, rows), F32)
        for stage, offsets in enumerate(TAKES):
            arrived(ag.at[number, pl.ds(0, len(offsets) - (0 in offsets))], 12 + stage, number)
            lows = []
            for offset in offsets:
                piece = piece_at(offset)
                direction = ag[number, piece].astype(F32)
                if ratio is not None:
                    direction += ratio * dir_ref[piece]
                low = direction.astype(BF16)
                dir_ref[piece] = direction
                dirb_ref[piece] = low
                lows.append((piece, low))
            for piece, low in lows:
                own += lax.dot_general(low, xh[0, piece], NT, preferred_element_type=F32)
                pair += lax.dot_general(low, xh[1, piece], NT, preferred_element_type=F32)
                wide = low.astype(F32)
                squares += jnp.sum(wide * wide, axis=1, keepdims=True)
        img_send[number, 0] = pair
        img_send[number, 1] = own
        dd_send[number] = to_row([squares])
        send(img_send.at[number], img_recv.at[number], 6, number, partner)
        send(dd_send.at[number], dd_recv.at[number], 7, number, partner)
        arrived(dd_recv.at[number], 7, number)
        arrived(img_recv.at[number], 6, number)
        own = mask_own * (own + img_recv[number, 0])
        pair = mask_pair * (pair + img_recv[number, 1])
        img[0] = own
        img[1] = pair
        return own, pair, to_column(dd_send[number] + dd_recv[number], 0)

    zero = jnp.zeros((traits, 1), F32)
    total, _ = sum_for_owner(0, lambda piece: dir_ref[piece] + drecv[piece], zero, SPLIT)
    search = total / noise_var + jnp.sqrt(ridge) * nco[...]
    search_ref[...] = search
    norm, _ = share(0, search, zero)
    swap_res.wait_recv()
    swap_geno.wait_recv()
    own, pair, squares = image_of(0, None)
    vals[3] = jnp.broadcast_to(norm, (traits, 128))
    vals[5] = jnp.broadcast_to(squares, (traits, 128))

    def iterate(number, carry):
        own, pair = img[0], img[1]
        squares = vals[5][:, 0:1]
        own_low = own.astype(BF16)
        pair_low = pair.astype(BF16)
        bend = jnp.sum(own * own_low.astype(F32), axis=1, keepdims=True)
        bend += jnp.sum(pair * pair_low.astype(F32), axis=1, keepdims=True)

        def part_of(piece):
            part = lax.dot_general(own_low, xh[0, piece], NN, preferred_element_type=F32)
            return part + lax.dot_general(pair_low, xh[1, piece], NN, preferred_element_type=F32)

        total, bend = sum_for_owner(number, part_of, bend, False)
        norm_now = vals[3][:, 0:1]
        step = norm_now / (bend / noise_var + ridge * squares)
        applied = total / noise_var + ridge * dirb_ref[r].astype(F32)
        search = search_ref[...] - step * applied
        search_ref[...] = search
        norm_next, step = share(number, search, step)
        acc[...] += step[None] * dirb_ref[...].astype(F32)
        fitted[...] += step[None] * img[...]
        vals[3] = jnp.broadcast_to(norm_next, (traits, 128))
        vals[4] = jnp.broadcast_to(step, (traits, 128))
        own, pair, squares = image_of(number, norm_next / norm_now)
        vals[5] = jnp.broadcast_to(squares, (traits, 128))
        return carry

    lax.fori_loop(1, ITERS, iterate, 0)

    swap_acc = to_pair(acc, c_recv, 3)
    swap_dir = to_pair(dirb_ref, d_recv, 4)
    own, pair = img[0], img[1]
    squares = vals[5][:, 0:1]
    guess = vals[4][:, 0:1]
    left_own = pres[0] - fitted[0] - guess * own
    left_pair = pres[1] - fitted[1] - guess * pair

    def both(one, two):
        return jnp.sum(one, axis=1, keepdims=True) + jnp.sum(two, axis=1, keepdims=True)

    fin[z] = to_row(
        [
            both(own * own.astype(BF16).astype(F32), pair * pair.astype(BF16).astype(F32)),
            both(left_own * left_own, left_pair * left_pair),
            both(left_own * own, left_pair * pair),
            both(own * own, pair * pair),
        ]
    )
    half_way = chips // 2
    for offset in sorted(range(1, chips), key=lambda o: -min(o, chips - o)):
        pltpu.make_async_remote_copy(
            src_ref=fin.at[z],
            dst_ref=fin.at[z],
            send_sem=pair_send.at[5],
            recv_sem=pair_recv.at[5],
            device_id=chip(offset if offset <= half_way else offset - chips, k),
            device_id_type=MESH,
        ).start()
    swap_acc.start()
    swap_dir.start()
    present = jnp.int32(0)
    for device in range(chips * CORES):
        present += s_counts[device]
    others = fin.at[pl.ds(0, chips - 1)]
    pltpu.make_async_copy(others, others, pair_recv.at[5]).wait()
    line = fin[0]
    for place in range(1, chips):
        line += fin[place]
    norm_now = vals[3][:, 0:1]
    step = norm_now / (to_column(line, 0) / noise_var + ridge * squares)
    shift = step - guess
    left = to_column(line, 1) - 2.0 * shift * to_column(line, 2) + shift * shift * to_column(line, 3)
    scale = (present.astype(F32) + PRIOR_DOF) * vals[2][:, 0:1]
    sigma_out[...] = to_row([(left + PRIOR_DOF * PRIOR_SCALE) / scale])
    resid_out[...] = pres[0] - (fitted[0] + step * own)
    for piece in range(NEAR):
        at = pl.multiple_of(mine + piece * width, width)
        coef_out[:, pl.ds(at, width)] = acc[piece] + step * dirb_ref[piece].astype(F32)
    swap_acc.wait_recv()
    swap_dir.wait_recv()
    for piece in range(NEAR):
        at = pl.multiple_of(other + piece * width, width)
        coef_out[:, pl.ds(at, width)] = c_recv[piece] + step * d_recv[piece].astype(F32)

    for swap in (swap_sum, swap_res, swap_geno, swap_acc, swap_dir):
        swap.wait_send()
    pltpu.make_async_copy(others, others, pair_send.at[5]).wait()

    def sent(ref, stage, number):
        pltpu.make_async_copy(ref, ref, st_send.at[number, stage]).wait()

    def drain(number, carry):
        sent(rs_recv.at[number], 0, number)
        sent(cv_recv.at[number], 1, number)
        for stage in (2, 8, 10):
            sent(mid.at[number, 0], stage, number)
            sent(mcv.at[number, 0], stage + 1, number)
        sent(agn.at[number, pl.ds(0, CORES * NEAR - 1)], 5, number)
        sent(img_recv.at[number], 6, number)
        sent(dd_recv.at[number], 7, number)
        for stage, offsets in enumerate(TAKES):
            sent(ag.at[number, pl.ds(0, len(offsets) - (0 in offsets))], 12 + stage, number)
        return carry

    lax.fori_loop(0, ITERS, drain, 0)


def update(geno, resid, npeople, ncoef, coef, block, prior, sigma, gamma, counts):
    rows, batch = geno.shape
    traits = resid.shape[0]
    devices = lax.axis_size(AXIS)
    chips = devices // CORES
    half = batch // CORES
    width = half // NEAR
    groups = chips // NEAR
    outside = pl.BlockSpec(memory_space=pltpu.HBM)
    inside = pl.BlockSpec(memory_space=pltpu.VMEM)
    block16 = (NEAR, traits, width)
    return pl.pallas_call(
        functools.partial(kernel, chips),
        name="gibbs",
        out_shape=(
            jax.ShapeDtypeStruct((traits, batch), F32),
            jax.ShapeDtypeStruct((traits, rows), F32),
            jax.ShapeDtypeStruct((1, 128), F32),
        ),
        in_specs=[outside] * 10,
        out_specs=(inside,) * 3,
        scratch_shapes=[
            pltpu.VMEM((2, NEAR, rows, width), BF16),
            pltpu.VMEM((NEAR, rows, width), BF16),
            pltpu.VMEM((4, traits, half), F32),
            pltpu.VMEM((traits, rows), F32),
            pltpu.VMEM((traits, rows), F32),
            pltpu.VMEM((traits, width), F32),
            pltpu.SMEM((1,), jnp.int32),
            pltpu.SMEM((traits,), F32),
            pltpu.SMEM((traits,), F32),
            pltpu.SMEM((traits,), F32),
            pltpu.SMEM((devices,), jnp.int32),
            pltpu.VMEM((2, traits, rows), F32),
            pltpu.VMEM(block16, F32),
            pltpu.VMEM(block16, F32),
            pltpu.VMEM((traits, width), F32),
            pltpu.VMEM((ITERS, *block16), jnp.int16),
            pltpu.VMEM((ITERS, 7, traits, width), jnp.int16),
            pltpu.VMEM((ITERS, NEAR, 1, 128), F32),
            pltpu.VMEM((ITERS, 8, 1, 128), F32),
            pltpu.VMEM((ITERS, groups, traits, width), jnp.int16),
            pltpu.VMEM((ITERS, groups, 1, 128), F32),
            pltpu.VMEM((ITERS, *block16), BF16),
            pltpu.VMEM((ITERS, CORES * NEAR, 1, 128), F32),
            pltpu.VMEM((ITERS, 1, 128), F32),
            pltpu.VMEM((traits, width), F32),
            pltpu.VMEM(block16, F32),
            pltpu.VMEM(block16, BF16),
            pltpu.VMEM(block16, F32),
            pltpu.VMEM((ITERS, 2, traits, rows), F32),
            pltpu.VMEM((ITERS, 2, traits, rows), F32),
            pltpu.VMEM((ITERS, 1, 128), F32),
            pltpu.VMEM((ITERS, 1, 128), F32),
            pltpu.VMEM((2, traits, rows), F32),
            pltpu.VMEM((2, traits, rows), F32),
            pltpu.VMEM((chips, 1, 128), F32),
            pltpu.VMEM(block16, F32),
            pltpu.VMEM(block16, BF16),
            pltpu.VMEM((6, traits, 128), F32),
            pltpu.SemaphoreType.DMA((23,)),
            pltpu.SemaphoreType.DMA((5,)),
            pltpu.SemaphoreType.DMA((6,)),
            pltpu.SemaphoreType.DMA((6,)),
            pltpu.SemaphoreType.DMA((ITERS, 15)),
            pltpu.SemaphoreType.DMA((ITERS, 15)),
        ],
        compiler_params=pltpu.CompilerParams(
            collective_id=0, has_side_effects=True, vmem_limit_bytes=67043328
        ),
    )(geno, resid, npeople, ncoef, coef, block, prior, sigma, gamma, counts)


def per_device(geno, resid, npeople, ncoef, coef, block, prior, sigma, gamma, counts):
    batch = geno.shape[1]
    batch_coef, resid_new, sigma_line = update(
        geno, resid, npeople, ncoef, coef, block, prior, sigma, gamma, counts
    )
    coef_new = lax.dynamic_update_slice_in_dim(coef, batch_coef, block[0] * batch, 1)
    return coef_new, resid_new, sigma_line[0, : resid.shape[0]]


def solution(mesh):
    return jax.shard_map(
        per_device,
        mesh=mesh,
        in_specs=(
            P(("trait", "ppl"), None),
            P("trait", "ppl"),
            P("trait", "ppl"),
            P("trait", None),
            P("trait", None),
            P("trait"),
            P("trait"),
            P("trait"),
            P("trait"),
            P("trait"),
        ),
        out_specs=(P("trait", None), P("trait", "ppl"), P("trait")),
        check_vma=False,
    )
```

```python
import functools

import jax
import jax.numpy as jnp
from jax import lax
from jax.experimental import pallas as pl
from jax.experimental.pallas import tpu as pltpu
from jax.sharding import PartitionSpec as P

ITERS = 4
PRIOR_DOF = 4.0
PRIOR_SCALE = 0.5
AXIS = "ppl"
CORES = 2
NEAR = 8
MESH = pl.DeviceIdType.MESH
F32 = jnp.float32
BF16 = jnp.bfloat16
NT = (((1,), (1,)), ((), ()))
NN = (((1,), (0,)), ((), ()))
CODES = 32000.0
FULL = (3, -3, 2, -2, 1, -1)
ENDS = (NEAR // 2, -(NEAR // 2))
SENDS = ((NEAR // 2, 3, -3), (2, -2), (1, -1), (0,))
TAKES = ((0, 1, -1), (2, -2), (3, -3, NEAR // 2))
TAKE_OF = {sign * abs(o): 12 + i for i, offsets in enumerate(TAKES) for o in offsets for sign in (1, -1)}


def kernel(
    chips,
    geno,
    resid,
    npeople,
    ncoef,
    coef,
    block,
    prior,
    sigma,
    gamma,
    counts,
    coef_out,
    resid_out,
    sigma_out,
    xh,
    xo,
    cf,
    res,
    npl,
    nco,
    s_block,
    s_prior,
    s_sigma,
    s_gamma,
    s_counts,
    pres,
    dsend,
    drecv,
    rs_own,
    rs_send,
    rs_recv,
    cv_send,
    cv_recv,
    mid,
    mcv,
    ag,
    agn,
    pn_send,
    pn_recv,
    search_ref,
    dir_ref,
    dirb_ref,
    acc,
    img_send,
    img_recv,
    dd_send,
    dd_recv,
    img,
    fitted,
    fin,
    c_recv,
    d_recv,
    vals,
    load_sem,
    small_sem,
    pair_send,
    pair_recv,
    st_send,
    st_recv,
):
    traits, rows = res.shape
    width = xo.shape[2]
    half = NEAR * width
    groups = chips // NEAR
    top = traits // 2
    me = lax.axis_index(AXIS)
    z = me // CORES
    k = lax.rem(me, CORES)
    g = z // NEAR
    r = lax.rem(z, NEAR)
    role = lax.rem(k + z // (NEAR // 2), CORES)
    partner = {AXIS: z * CORES + (1 - k)}

    def chip(offset):
        there = lax.rem(z + offset + chips, chips)
        return {AXIS: there * CORES + lax.rem(role + there // (NEAR // 2), CORES)}

    def piece_at(offset):
        return lax.rem(r + offset + NEAR, NEAR)

    barrier = pltpu.get_barrier_semaphore()
    for target in (*[chip(offset) for offset in (*ENDS, *FULL)], partner):
        pl.semaphore_signal(barrier, inc=1, device_id=target, device_id_type=MESH)

    mine = pl.multiple_of(role * half, half)
    other = pl.multiple_of((1 - role) * half, half)
    own_col = pl.multiple_of(role * half + r * width, width)
    loads = [
        pltpu.make_async_copy(coef.at[:, pl.ds(mine, half)], cf.at[0], load_sem.at[0]),
        pltpu.make_async_copy(coef.at[:, pl.ds(other, half)], cf.at[1], load_sem.at[1]),
        pltpu.make_async_copy(coef.at[:, pl.ds(2 * half + mine, half)], cf.at[2], load_sem.at[2]),
        pltpu.make_async_copy(coef.at[:, pl.ds(2 * half + other, half)], cf.at[3], load_sem.at[3]),
        pltpu.make_async_copy(resid, res, load_sem.at[4]),
        pltpu.make_async_copy(npeople, npl, load_sem.at[5]),
        pltpu.make_async_copy(ncoef.at[:, pl.ds(own_col, width)], nco, load_sem.at[6]),
    ]
    for piece in range(NEAR):
        at = pl.multiple_of(mine + piece * width, width)
        loads.append(
            pltpu.make_async_copy(geno.at[:, pl.ds(at, width)], xh.at[0, piece], load_sem.at[7 + piece])
        )
    for piece in range(NEAR):
        at = pl.multiple_of(other + piece * width, width)
        loads.append(
            pltpu.make_async_copy(geno.at[:, pl.ds(at, width)], xo.at[piece], load_sem.at[15 + piece])
        )
    smalls = [
        pltpu.make_async_copy(block, s_block, small_sem.at[0]),
        pltpu.make_async_copy(prior, s_prior, small_sem.at[1]),
        pltpu.make_async_copy(sigma, s_sigma, small_sem.at[2]),
        pltpu.make_async_copy(gamma, s_gamma, small_sem.at[3]),
        pltpu.make_async_copy(counts, s_counts, small_sem.at[4]),
    ]
    for copy in smalls + loads:
        copy.start()
    for copy in smalls:
        copy.wait()

    row_id = lax.broadcasted_iota(jnp.int32, (traits, 128), 0)
    lane_id = lax.broadcasted_iota(jnp.int32, (traits, 128), 1)

    def to_row(columns):
        total = jnp.zeros((traits, 128), F32)
        for place, column in enumerate(columns):
            total += jnp.where(lane_id == row_id + place * traits, column, 0.0)
        return jnp.sum(total, axis=0, keepdims=True)

    def to_column(line, place):
        return jnp.sum(
            jnp.where(lane_id == row_id + place * traits, line, 0.0), axis=1, keepdims=True
        )

    def column_of(ref):
        column = jnp.zeros((traits, 128), F32)
        for trait in range(traits):
            column = jnp.where(row_id == trait, ref[trait], column)
        return column

    vals[0] = column_of(s_sigma)
    vals[1] = column_of(s_prior)
    vals[2] = column_of(s_gamma)
    noise_var = vals[0][:, 0:1]
    ridge = vals[1][:, 0:1]
    slot = lax.broadcasted_iota(jnp.int32, (traits, rows), 1)
    mask_own = (slot < s_counts[me]).astype(F32)
    mask_pair = (slot < s_counts[z * CORES + (1 - k)]).astype(F32)

    def coded(values):
        largest = jnp.maximum(jnp.max(jnp.abs(values), axis=1, keepdims=True), 1e-30)
        codes = jnp.round(values * (CODES / largest)).astype(jnp.int32).astype(jnp.int16)
        return codes, largest * (1.0 / CODES)

    def decoded(codes, unit):
        return codes.astype(jnp.int32).astype(F32) * unit

    for copy in loads:
        copy.wait()
    first = s_block[0] == 0
    old_mine = jnp.where(first, cf[0], cf[2]).astype(BF16)
    old_other = jnp.where(first, cf[1], cf[3]).astype(BF16)
    fitted_old = jnp.zeros((traits, rows), F32)
    for piece in range(NEAR):
        columns = slice(piece * width, (piece + 1) * width)
        fitted_old += lax.dot_general(old_mine[:, columns], xh[0, piece], NT, preferred_element_type=F32)
        fitted_old += lax.dot_general(old_other[:, columns], xo[piece], NT, preferred_element_type=F32)
    partial_res = mask_own * (res[...] + fitted_old)
    pres[0] = partial_res
    target = (mask_own * (partial_res + jnp.sqrt(noise_var) * npl[...])).astype(BF16)
    for piece in range(NEAR):
        dsend[piece] = lax.dot_general(target, xo[piece], NN, preferred_element_type=F32)
    for piece in range(NEAR):
        dir_ref[piece] = lax.dot_general(target, xh[0, piece], NN, preferred_element_type=F32)
    fitted[...] = jnp.zeros_like(fitted)
    acc[...] = jnp.zeros_like(acc)

    pl.semaphore_wait(barrier, len(ENDS) + len(FULL) + 1)

    def to_pair(src, dst, index):
        return pltpu.make_async_remote_copy(
            src_ref=src,
            dst_ref=dst,
            send_sem=pair_send.at[index],
            recv_sem=pair_recv.at[index],
            device_id=partner,
            device_id_type=MESH,
        )

    swap_sum = to_pair(dsend, drecv, 0)
    swap_res = to_pair(pres.at[0], pres.at[1], 1)
    swap_geno = to_pair(xo, xh.at[1], 2)
    swap_sum.start()
    swap_res.start()
    swap_geno.start()
    swap_sum.wait_recv()

    def send(src, dst, stage, number, target):
        pltpu.make_async_remote_copy(
            src_ref=src,
            dst_ref=dst,
            send_sem=st_send.at[number, stage],
            recv_sem=st_recv.at[number, stage],
            device_id=target,
            device_id_type=MESH,
        ).start()

    def arrived(ref, stage, number):
        pltpu.make_async_copy(ref, ref, st_recv.at[number, stage]).wait()

    def sum_for_owner(number, part_of, column, relay):
        for offsets in SENDS:
            pieces = [piece_at(offset) for offset in offsets]
            for offset, piece, part in zip(offsets, pieces, [part_of(piece) for piece in pieces]):
                if offset == 0:
                    rs_own[...] = part
                    continue
                rs_send[number, piece], unit = coded(part)
                cv_send[number, piece] = to_row([column, unit])
            for offset, piece in zip(offsets, pieces):
                line = cv_send.at[number, piece]
                codes = rs_send.at[number, piece]
                if offset == ENDS[0]:
                    for place, end in enumerate(ENDS):
                        band = pl.ds(place * top, top)
                        send(line, cv_recv.at[number, 6 + place], 1, number, chip(end))
                        send(
                            codes.at[band], rs_recv.at[number, 6, band], 0, number, chip(end)
                        )
                elif offset:
                    slot_id = FULL.index(offset)
                    send(line, cv_recv.at[number, slot_id], 1, number, chip(offset))
                    send(codes, rs_recv.at[number, slot_id], 0, number, chip(offset))
        arrived(cv_recv.at[number], 1, number)
        sums = to_row([column])
        for slot_id in range(7):
            sums += cv_recv[number, slot_id]
        sums = to_column(sums, 0)
        upper = lax.broadcasted_iota(jnp.int32, (traits, 1), 0) < top
        arrived(rs_recv.at[number], 0, number)
        total = rs_own[...]
        for slot_id in range(6):
            total += decoded(rs_recv[number, slot_id], to_column(cv_recv[number, slot_id], 1))
        unit = jnp.where(upper, to_column(cv_recv[number, 6], 1), to_column(cv_recv[number, 7], 1))
        total += decoded(rs_recv[number, 6], unit)
        mid[number, g], unit = coded(total)
        mcv[number, g] = to_row([sums, unit])

        def pass_on(group, offset, stage):
            send(mcv.at[number, group], mcv.at[number, group], stage + 1, number, chip(offset))
            send(mid.at[number, group], mid.at[number, group], stage, number, chip(offset))

        if not relay:
            pass_on(g, 2 * NEAR, 10)
        pass_on(g, NEAR, 2)
        pass_on(g, -NEAR, 8)
        arrived(mcv.at[number, 0], 9, number)
        arrived(mid.at[number, 0], 8, number)
        if relay:
            pass_on(lax.rem(g + 1, groups), -NEAR, 10)
        arrived(mcv.at[number, 0], 3, number)
        arrived(mid.at[number, 0], 2, number)
        arrived(mcv.at[number, 0], 11, number)
        arrived(mid.at[number, 0], 10, number)
        sums = mcv[number, 0]
        total = decoded(mid[number, 0], to_column(sums, 1))
        for group in range(1, groups):
            line = mcv[number, group]
            sums += line
            total += decoded(mid[number, group], to_column(line, 1))
        return total, to_column(sums, 0)

    def share(number, search, step):
        ag[number, r] = search.astype(BF16)
        for place, end in enumerate(ENDS):
            band = pl.ds(place * top, top)
            send(ag.at[number, r, band], ag.at[number, r, band], TAKE_OF[end], number, chip(end))
        for offset in FULL:
            send(ag.at[number, r], ag.at[number, r], TAKE_OF[offset], number, chip(offset))
        pn_send[number] = to_row([jnp.sum(search * search, axis=1, keepdims=True), step])
        send(pn_send.at[number], pn_recv.at[number], 15, number, partner)
        arrived(pn_recv.at[number], 15, number)
        here, there = pn_send[number], pn_recv[number]
        steps = jnp.where(role == 0, here, there)
        agn[number, r] = jnp.where(lane_id[0:1] < traits, here + there, steps)
        for offset in (ENDS[0], *FULL):
            send(agn.at[number, r], agn.at[number, r], 5, number, chip(offset))
        arrived(agn.at[number, pl.ds(0, NEAR - 1)], 5, number)
        line = agn[number, 0]
        for place in range(1, NEAR):
            line += agn[number, place]
        return to_column(line, 0), to_column(agn[number, 0], 1)

    def image_of(number, ratio):
        squares = jnp.zeros((traits, 1), F32)
        own = jnp.zeros((traits, rows), F32)
        pair = jnp.zeros((traits, rows), F32)
        for stage, offsets in enumerate(TAKES):
            arrived(ag.at[number, pl.ds(0, len(offsets) - (0 in offsets))], 12 + stage, number)
            lows = []
            for offset in offsets:
                piece = piece_at(offset)
                direction = ag[number, piece].astype(F32)
                if ratio is not None:
                    direction += ratio * dir_ref[piece]
                low = direction.astype(BF16)
                dir_ref[piece] = direction
                dirb_ref[piece] = low
                lows.append((piece, low))
            for piece, low in lows:
                own += lax.dot_general(low, xh[0, piece], NT, preferred_element_type=F32)
                pair += lax.dot_general(low, xh[1, piece], NT, preferred_element_type=F32)
                wide = low.astype(F32)
                squares += jnp.sum(wide * wide, axis=1, keepdims=True)
        img_send[number, 0] = pair
        img_send[number, 1] = own
        dd_send[number] = to_row([squares])
        send(img_send.at[number], img_recv.at[number], 6, number, partner)
        send(dd_send.at[number], dd_recv.at[number], 7, number, partner)
        arrived(dd_recv.at[number], 7, number)
        arrived(img_recv.at[number], 6, number)
        own = mask_own * (own + img_recv[number, 0])
        pair = mask_pair * (pair + img_recv[number, 1])
        img[0] = own
        img[1] = pair
        return own, pair, to_column(dd_send[number] + dd_recv[number], 0)

    zero = jnp.zeros((traits, 1), F32)
    total, _ = sum_for_owner(0, lambda piece: dir_ref[piece] + drecv[piece], zero, True)
    search = total / noise_var + jnp.sqrt(ridge) * nco[...]
    search_ref[...] = search
    norm, _ = share(0, search, zero)
    swap_res.wait_recv()
    swap_geno.wait_recv()
    own, pair, squares = image_of(0, None)
    vals[3] = jnp.broadcast_to(norm, (traits, 128))
    vals[5] = jnp.broadcast_to(squares, (traits, 128))

    def iterate(number, carry):
        own, pair = img[0], img[1]
        squares = vals[5][:, 0:1]
        own_low = own.astype(BF16)
        pair_low = pair.astype(BF16)
        bend = jnp.sum(own * own_low.astype(F32), axis=1, keepdims=True)
        bend += jnp.sum(pair * pair_low.astype(F32), axis=1, keepdims=True)

        def part_of(piece):
            part = lax.dot_general(own_low, xh[0, piece], NN, preferred_element_type=F32)
            return part + lax.dot_general(pair_low, xh[1, piece], NN, preferred_element_type=F32)

        total, bend = sum_for_owner(number, part_of, bend, False)
        norm_now = vals[3][:, 0:1]
        step = norm_now / (bend / noise_var + ridge * squares)
        applied = total / noise_var + ridge * dirb_ref[r].astype(F32)
        search = search_ref[...] - step * applied
        search_ref[...] = search
        norm_next, step = share(number, search, step)
        acc[...] += step[None] * dirb_ref[...].astype(F32)
        fitted[...] += step[None] * img[...]
        vals[3] = jnp.broadcast_to(norm_next, (traits, 128))
        vals[4] = jnp.broadcast_to(step, (traits, 128))
        own, pair, squares = image_of(number, norm_next / norm_now)
        vals[5] = jnp.broadcast_to(squares, (traits, 128))
        return carry

    lax.fori_loop(1, ITERS, iterate, 0)

    swap_acc = to_pair(acc, c_recv, 3)
    swap_dir = to_pair(dirb_ref, d_recv, 4)
    own, pair = img[0], img[1]
    squares = vals[5][:, 0:1]
    guess = vals[4][:, 0:1]
    left_own = pres[0] - fitted[0] - guess * own
    left_pair = pres[1] - fitted[1] - guess * pair

    def both(one, two):
        return jnp.sum(one, axis=1, keepdims=True) + jnp.sum(two, axis=1, keepdims=True)

    fin[z] = to_row(
        [
            both(own * own.astype(BF16).astype(F32), pair * pair.astype(BF16).astype(F32)),
            both(left_own * left_own, left_pair * left_pair),
            both(left_own * own, left_pair * pair),
            both(own * own, pair * pair),
        ]
    )
    half_way = chips // 2
    for offset in sorted(range(1, chips), key=lambda o: -min(o, chips - o)):
        pltpu.make_async_remote_copy(
            src_ref=fin.at[z],
            dst_ref=fin.at[z],
            send_sem=pair_send.at[5],
            recv_sem=pair_recv.at[5],
            device_id=chip(offset if offset <= half_way else offset - chips),
            device_id_type=MESH,
        ).start()
    swap_acc.start()
    swap_dir.start()
    present = jnp.int32(0)
    for device in range(chips * CORES):
        present += s_counts[device]
    others = fin.at[pl.ds(0, chips - 1)]
    pltpu.make_async_copy(others, others, pair_recv.at[5]).wait()
    line = fin[0]
    for place in range(1, chips):
        line += fin[place]
    norm_now = vals[3][:, 0:1]
    step = norm_now / (to_column(line, 0) / noise_var + ridge * squares)
    shift = step - guess
    left = to_column(line, 1) - 2.0 * shift * to_column(line, 2) + shift * shift * to_column(line, 3)
    scale = (present.astype(F32) + PRIOR_DOF) * vals[2][:, 0:1]
    sigma_out[...] = to_row([(left + PRIOR_DOF * PRIOR_SCALE) / scale])
    resid_out[...] = pres[0] - (fitted[0] + step * own)

    def put(start, place, steps, directions):
        for piece in range(NEAR):
            columns = slice(piece * width, (piece + 1) * width)
            new = steps[piece] + step * directions[piece].astype(F32)
            at = pl.multiple_of(start + piece * width, width)
            coef_out[:, pl.ds(at, width)] = jnp.where(first, new, cf[place, :, columns])
            at = pl.multiple_of(CORES * half + start + piece * width, width)
            coef_out[:, pl.ds(at, width)] = jnp.where(first, cf[place + 2, :, columns], new)

    put(mine, 0, acc, dirb_ref)
    swap_acc.wait_recv()
    swap_dir.wait_recv()
    put(other, 1, c_recv, d_recv)

    for swap in (swap_sum, swap_res, swap_geno, swap_acc, swap_dir):
        swap.wait_send()
    pltpu.make_async_copy(others, others, pair_send.at[5]).wait()

    def sent(ref, stage, number):
        pltpu.make_async_copy(ref, ref, st_send.at[number, stage]).wait()

    def drain(number, carry):
        sent(rs_recv.at[number], 0, number)
        sent(cv_recv.at[number], 1, number)
        for stage in (2, 8, 10):
            sent(mid.at[number, 0], stage, number)
            sent(mcv.at[number, 0], stage + 1, number)
        sent(agn.at[number, pl.ds(0, NEAR - 1)], 5, number)
        sent(pn_recv.at[number], 15, number)
        sent(img_recv.at[number], 6, number)
        sent(dd_recv.at[number], 7, number)
        for stage, offsets in enumerate(TAKES):
            sent(ag.at[number, pl.ds(0, len(offsets) - (0 in offsets))], 12 + stage, number)
        return carry

    lax.fori_loop(0, ITERS, drain, 0)


def update(geno, resid, npeople, ncoef, coef, block, prior, sigma, gamma, counts):
    rows, batch = geno.shape
    traits = resid.shape[0]
    devices = lax.axis_size(AXIS)
    chips = devices // CORES
    half = batch // CORES
    width = half // NEAR
    groups = chips // NEAR
    outside = pl.BlockSpec(memory_space=pltpu.HBM)
    inside = pl.BlockSpec(memory_space=pltpu.VMEM)
    block16 = (NEAR, traits, width)
    return pl.pallas_call(
        functools.partial(kernel, chips),
        name="gibbs",
        out_shape=(
            jax.ShapeDtypeStruct(coef.shape, F32),
            jax.ShapeDtypeStruct((traits, rows), F32),
            jax.ShapeDtypeStruct((1, 128), F32),
        ),
        in_specs=[outside] * 10,
        out_specs=(inside,) * 3,
        scratch_shapes=[
            pltpu.VMEM((2, NEAR, rows, width), BF16),
            pltpu.VMEM((NEAR, rows, width), BF16),
            pltpu.VMEM((4, traits, half), F32),
            pltpu.VMEM((traits, rows), F32),
            pltpu.VMEM((traits, rows), F32),
            pltpu.VMEM((traits, width), F32),
            pltpu.SMEM((1,), jnp.int32),
            pltpu.SMEM((traits,), F32),
            pltpu.SMEM((traits,), F32),
            pltpu.SMEM((traits,), F32),
            pltpu.SMEM((devices,), jnp.int32),
            pltpu.VMEM((2, traits, rows), F32),
            pltpu.VMEM(block16, F32),
            pltpu.VMEM(block16, F32),
            pltpu.VMEM((traits, width), F32),
            pltpu.VMEM((ITERS, *block16), jnp.int16),
            pltpu.VMEM((ITERS, 7, traits, width), jnp.int16),
            pltpu.VMEM((ITERS, NEAR, 1, 128), F32),
            pltpu.VMEM((ITERS, 8, 1, 128), F32),
            pltpu.VMEM((ITERS, groups, traits, width), jnp.int16),
            pltpu.VMEM((ITERS, groups, 1, 128), F32),
            pltpu.VMEM((ITERS, *block16), BF16),
            pltpu.VMEM((ITERS, NEAR, 1, 128), F32),
            pltpu.VMEM((ITERS, 1, 128), F32),
            pltpu.VMEM((ITERS, 1, 128), F32),
            pltpu.VMEM((traits, width), F32),
            pltpu.VMEM(block16, F32),
            pltpu.VMEM(block16, BF16),
            pltpu.VMEM(block16, F32),
            pltpu.VMEM((ITERS, 2, traits, rows), F32),
            pltpu.VMEM((ITERS, 2, traits, rows), F32),
            pltpu.VMEM((ITERS, 1, 128), F32),
            pltpu.VMEM((ITERS, 1, 128), F32),
            pltpu.VMEM((2, traits, rows), F32),
            pltpu.VMEM((2, traits, rows), F32),
            pltpu.VMEM((chips, 1, 128), F32),
            pltpu.VMEM(block16, F32),
            pltpu.VMEM(block16, BF16),
            pltpu.VMEM((6, traits, 128), F32),
            pltpu.SemaphoreType.DMA((23,)),
            pltpu.SemaphoreType.DMA((5,)),
            pltpu.SemaphoreType.DMA((6,)),
            pltpu.SemaphoreType.DMA((6,)),
            pltpu.SemaphoreType.DMA((ITERS, 16)),
            pltpu.SemaphoreType.DMA((ITERS, 16)),
        ],
        compiler_params=pltpu.CompilerParams(
            collective_id=0, has_side_effects=True, vmem_limit_bytes=64 * 1024 * 1000
        ),
    )(geno, resid, npeople, ncoef, coef, block, prior, sigma, gamma, counts)


def per_device(geno, resid, npeople, ncoef, coef, block, prior, sigma, gamma, counts):
    coef_new, resid_new, sigma_line = update(
        geno, resid, npeople, ncoef, coef, block, prior, sigma, gamma, counts
    )
    return coef_new, resid_new, sigma_line[0, : resid.shape[0]]


def solution(mesh):
    return jax.shard_map(
        per_device,
        mesh=mesh,
        in_specs=(
            P(("trait", "ppl"), None),
            P("trait", "ppl"),
            P("trait", "ppl"),
            P("trait", None),
            P("trait", None),
            P("trait"),
            P("trait"),
            P("trait"),
            P("trait"),
            P("trait"),
        ),
        out_specs=(P("trait", None), P("trait", "ppl"), P("trait")),
        check_vma=False,
    )
```

```python
import functools

import jax
import jax.numpy as jnp
from jax import lax
from jax.experimental import pallas as pl
from jax.experimental.pallas import tpu as pltpu
from jax.sharding import PartitionSpec as P

ITERS = 4
PRIOR_DOF = 4.0
PRIOR_SCALE = 0.5
AXIS = "ppl"
CORES = 2
NEAR = 8
MESH = pl.DeviceIdType.MESH
F32 = jnp.float32
BF16 = jnp.bfloat16
NT = (((1,), (1,)), ((), ()))
NN = (((1,), (0,)), ((), ()))
CODES = 32000.0
FULL = (3, -3, 2, -2, 1, -1)
ENDS = (NEAR // 2, -(NEAR // 2))
SENDS = ((NEAR // 2, 3, -3), (2, -2), (1, -1), (0,))
TAKES = ((0, 1, -1), (2, -2), (3, -3, NEAR // 2))
TAKE_OF = {sign * abs(o): 12 + i for i, offsets in enumerate(TAKES) for o in offsets for sign in (1, -1)}


def kernel(
    chips,
    geno,
    resid,
    npeople,
    ncoef,
    coef,
    block,
    prior,
    sigma,
    gamma,
    counts,
    coef_out,
    resid_out,
    sigma_out,
    xh,
    xo,
    cf,
    res,
    npl,
    nco,
    s_block,
    s_prior,
    s_sigma,
    s_gamma,
    s_counts,
    pres,
    dsend,
    drecv,
    rs_own,
    rs_send,
    rs_recv,
    cv_send,
    cv_recv,
    mid,
    mcv,
    ag,
    agn,
    search_ref,
    dir_ref,
    acc,
    img_send,
    img_recv,
    dd_send,
    dd_recv,
    img,
    fitted,
    fin,
    c_recv,
    d_recv,
    vals,
    load_sem,
    small_sem,
    pair_send,
    pair_recv,
    st_send,
    st_recv,
):
    traits, rows = res.shape
    width = xo.shape[2]
    half = NEAR * width
    groups = chips // NEAR
    top = traits // 2
    me = lax.axis_index(AXIS)
    z = me // CORES
    k = lax.rem(me, CORES)
    g = z // NEAR
    r = lax.rem(z, NEAR)
    partner = {AXIS: z * CORES + (1 - k)}

    def chip(offset):
        return {AXIS: lax.rem(z + offset + chips, chips) * CORES + k}

    def piece_at(offset):
        return lax.rem(r + offset + NEAR, NEAR)

    barrier = pltpu.get_barrier_semaphore()
    for target in (*[chip(offset) for offset in (*ENDS, *FULL)], partner):
        pl.semaphore_signal(barrier, inc=1, device_id=target, device_id_type=MESH)

    mine = pl.multiple_of(k * half, half)
    other = pl.multiple_of((1 - k) * half, half)
    own_col = pl.multiple_of(k * half + r * width, width)
    loads = [
        pltpu.make_async_copy(coef.at[:, pl.ds(mine, half)], cf.at[0], load_sem.at[0]),
        pltpu.make_async_copy(coef.at[:, pl.ds(other, half)], cf.at[1], load_sem.at[1]),
        pltpu.make_async_copy(coef.at[:, pl.ds(2 * half + mine, half)], cf.at[2], load_sem.at[2]),
        pltpu.make_async_copy(coef.at[:, pl.ds(2 * half + other, half)], cf.at[3], load_sem.at[3]),
        pltpu.make_async_copy(resid, res, load_sem.at[4]),
        pltpu.make_async_copy(npeople, npl, load_sem.at[5]),
        pltpu.make_async_copy(ncoef.at[:, pl.ds(own_col, width)], nco, load_sem.at[6]),
    ]
    for piece in range(NEAR):
        at = pl.multiple_of(mine + piece * width, width)
        loads.append(
            pltpu.make_async_copy(geno.at[:, pl.ds(at, width)], xh.at[0, piece], load_sem.at[7 + piece])
        )
    for piece in range(NEAR):
        at = pl.multiple_of(other + piece * width, width)
        loads.append(
            pltpu.make_async_copy(geno.at[:, pl.ds(at, width)], xo.at[piece], load_sem.at[15 + piece])
        )
    smalls = [
        pltpu.make_async_copy(block, s_block, small_sem.at[0]),
        pltpu.make_async_copy(prior, s_prior, small_sem.at[1]),
        pltpu.make_async_copy(sigma, s_sigma, small_sem.at[2]),
        pltpu.make_async_copy(gamma, s_gamma, small_sem.at[3]),
        pltpu.make_async_copy(counts, s_counts, small_sem.at[4]),
    ]
    for copy in smalls + loads:
        copy.start()
    for copy in smalls:
        copy.wait()

    row_id = lax.broadcasted_iota(jnp.int32, (traits, 128), 0)
    lane_id = lax.broadcasted_iota(jnp.int32, (traits, 128), 1)

    def to_row(columns):
        total = jnp.zeros((traits, 128), F32)
        for place, column in enumerate(columns):
            total += jnp.where(lane_id == row_id + place * traits, column, 0.0)
        return jnp.sum(total, axis=0, keepdims=True)

    def to_column(line, place):
        return jnp.sum(
            jnp.where(lane_id == row_id + place * traits, line, 0.0), axis=1, keepdims=True
        )

    def column_of(ref):
        column = jnp.zeros((traits, 128), F32)
        for trait in range(traits):
            column = jnp.where(row_id == trait, ref[trait], column)
        return column

    vals[0] = column_of(s_sigma)
    vals[1] = column_of(s_prior)
    vals[2] = column_of(s_gamma)
    noise_var = vals[0][:, 0:1]
    ridge = vals[1][:, 0:1]
    slot = lax.broadcasted_iota(jnp.int32, (traits, rows), 1)
    mask_own = (slot < s_counts[me]).astype(F32)
    mask_pair = (slot < s_counts[z * CORES + (1 - k)]).astype(F32)

    def coded(values):
        largest = jnp.maximum(jnp.max(jnp.abs(values), axis=1, keepdims=True), 1e-30)
        codes = jnp.round(values * (CODES / largest)).astype(jnp.int32).astype(jnp.int16)
        return codes, largest * (1.0 / CODES)

    def decoded(codes, unit):
        return codes.astype(jnp.int32).astype(F32) * unit

    for copy in loads:
        copy.wait()
    first = s_block[0] == 0
    old_mine = jnp.where(first, cf[0], cf[2]).astype(BF16)
    old_other = jnp.where(first, cf[1], cf[3]).astype(BF16)
    fitted_old = jnp.zeros((traits, rows), F32)
    for piece in range(NEAR):
        columns = slice(piece * width, (piece + 1) * width)
        fitted_old += lax.dot_general(old_mine[:, columns], xh[0, piece], NT, preferred_element_type=F32)
        fitted_old += lax.dot_general(old_other[:, columns], xo[piece], NT, preferred_element_type=F32)
    partial_res = mask_own * (res[...] + fitted_old)
    pres[0] = partial_res
    target = (mask_own * (partial_res + jnp.sqrt(noise_var) * npl[...])).astype(BF16)
    for piece in range(NEAR):
        dsend[piece] = lax.dot_general(target, xo[piece], NN, preferred_element_type=F32)
    for piece in range(NEAR):
        dir_ref[piece] = lax.dot_general(target, xh[0, piece], NN, preferred_element_type=F32)
    fitted[...] = jnp.zeros_like(fitted)
    acc[...] = jnp.zeros_like(acc)

    pl.semaphore_wait(barrier, len(ENDS) + len(FULL) + 1)

    def to_pair(src, dst, index):
        return pltpu.make_async_remote_copy(
            src_ref=src,
            dst_ref=dst,
            send_sem=pair_send.at[index],
            recv_sem=pair_recv.at[index],
            device_id=partner,
            device_id_type=MESH,
        )

    swap_sum = to_pair(dsend, drecv, 0)
    swap_res = to_pair(pres.at[0], pres.at[1], 1)
    swap_geno = to_pair(xo, xh.at[1], 2)
    swap_sum.start()
    swap_res.start()
    swap_geno.start()
    swap_sum.wait_recv()

    def send(src, dst, stage, number, target):
        pltpu.make_async_remote_copy(
            src_ref=src,
            dst_ref=dst,
            send_sem=st_send.at[number, stage],
            recv_sem=st_recv.at[number, stage],
            device_id=target,
            device_id_type=MESH,
        ).start()

    def arrived(ref, stage, number):
        pltpu.make_async_copy(ref, ref, st_recv.at[number, stage]).wait()

    def sum_for_owner(number, part_of, column, relay, meanwhile=lambda: None):
        for offsets in SENDS:
            pieces = [piece_at(offset) for offset in offsets]
            for offset, piece, part in zip(offsets, pieces, [part_of(piece) for piece in pieces]):
                if offset == 0:
                    rs_own[...] = part
                    continue
                rs_send[number, piece], unit = coded(part)
                cv_send[number, piece] = to_row([column, unit])
            for offset, piece in zip(offsets, pieces):
                line = cv_send.at[number, piece]
                codes = rs_send.at[number, piece]
                if offset == ENDS[0]:
                    for place, end in enumerate(ENDS):
                        band = pl.ds(place * top, top)
                        send(line, cv_recv.at[number, 6 + place], 1, number, chip(end))
                        send(
                            codes.at[band], rs_recv.at[number, 6, band], 0, number, chip(end)
                        )
                elif offset:
                    slot_id = FULL.index(offset)
                    send(line, cv_recv.at[number, slot_id], 1, number, chip(offset))
                    send(codes, rs_recv.at[number, slot_id], 0, number, chip(offset))
        meanwhile()
        arrived(cv_recv.at[number], 1, number)
        sums = to_row([column])
        for slot_id in range(7):
            sums += cv_recv[number, slot_id]
        sums = to_column(sums, 0)
        upper = lax.broadcasted_iota(jnp.int32, (traits, 1), 0) < top
        arrived(rs_recv.at[number], 0, number)
        total = rs_own[...]
        for slot_id in range(6):
            total += decoded(rs_recv[number, slot_id], to_column(cv_recv[number, slot_id], 1))
        unit = jnp.where(upper, to_column(cv_recv[number, 6], 1), to_column(cv_recv[number, 7], 1))
        total += decoded(rs_recv[number, 6], unit)
        mid[number, g], unit = coded(total)
        mcv[number, g] = to_row([sums, unit])

        def pass_on(group, offset, stage):
            send(mcv.at[number, group], mcv.at[number, group], stage + 1, number, chip(offset))
            send(mid.at[number, group], mid.at[number, group], stage, number, chip(offset))

        if not relay:
            pass_on(g, 2 * NEAR, 10)
        pass_on(g, NEAR, 2)
        pass_on(g, -NEAR, 8)
        arrived(mcv.at[number, 0], 9, number)
        arrived(mid.at[number, 0], 8, number)
        if relay:
            pass_on(lax.rem(g + 1, groups), -NEAR, 10)
        arrived(mcv.at[number, 0], 3, number)
        arrived(mid.at[number, 0], 2, number)
        arrived(mcv.at[number, 0], 11, number)
        arrived(mid.at[number, 0], 10, number)
        sums = mcv[number, 0]
        total = decoded(mid[number, 0], to_column(sums, 1))
        for group in range(1, groups):
            line = mcv[number, group]
            sums += line
            total += decoded(mid[number, group], to_column(line, 1))
        return total, to_column(sums, 0)

    def share(number, search, step):
        ag[number, r] = search.astype(BF16)
        agn[number, r] = to_row([jnp.sum(search * search, axis=1, keepdims=True), step])
        for place, end in enumerate(ENDS):
            band = pl.ds(place * top, top)
            send(ag.at[number, r, band], ag.at[number, r, band], TAKE_OF[end], number, chip(end))
            if place == 0:
                send(agn.at[number, r], agn.at[number, r], 5, number, chip(end))
        for offset in FULL:
            send(ag.at[number, r], ag.at[number, r], TAKE_OF[offset], number, chip(offset))
            send(agn.at[number, r], agn.at[number, r], 5, number, chip(offset))

    def image_of(number, fresh):
        own = jnp.zeros((traits, rows), F32)
        pair = jnp.zeros((traits, rows), F32)
        squares = jnp.zeros((traits, 1), F32)
        cross = jnp.zeros((traits, 1), F32)
        for stage, offsets in enumerate(TAKES):
            arrived(ag.at[number, pl.ds(0, len(offsets) - (0 in offsets))], 12 + stage, number)
            for offset in offsets:
                piece = piece_at(offset)
                low = ag[number, piece]
                own += lax.dot_general(low, xh[0, piece], NT, preferred_element_type=F32)
                pair += lax.dot_general(low, xh[1, piece], NT, preferred_element_type=F32)
                wide = low.astype(F32)
                squares += jnp.sum(wide * wide, axis=1, keepdims=True)
                if not fresh:
                    cross += jnp.sum(wide * dir_ref[piece], axis=1, keepdims=True)
        img_send[number, 0] = pair
        img_send[number, 1] = own
        send(img_send.at[number], img_recv.at[number], 6, number, partner)
        arrived(agn.at[number, pl.ds(0, NEAR - 1)], 5, number)
        line = agn[number, 0]
        for place in range(1, NEAR):
            line += agn[number, place]
        dd_send[number] = to_row([to_column(line, 0), squares, cross])
        send(dd_send.at[number], dd_recv.at[number], 7, number, partner)
        step = to_column(agn[number, 0], 1)
        if not fresh:
            fitted[...] += step[None] * img[...]
            acc[...] += step[None] * dir_ref[...]
        arrived(dd_recv.at[number], 7, number)
        line = dd_send[number] + dd_recv[number]
        norm = to_column(line, 0)
        squares = to_column(line, 1)
        arrived(img_recv.at[number], 6, number)
        own = mask_own * (own + img_recv[number, 0])
        pair = mask_pair * (pair + img_recv[number, 1])
        if fresh:
            ratio = jnp.zeros((traits, 1), F32)
        else:
            ratio = norm / vals[3][:, 0:1]
            own += ratio * img[0]
            pair += ratio * img[1]
            squares += ratio * (2.0 * to_column(line, 2) + ratio * vals[5][:, 0:1])
        img[0] = own
        img[1] = pair
        vals[3] = jnp.broadcast_to(norm, (traits, 128))
        vals[4] = jnp.broadcast_to(step, (traits, 128))
        vals[5] = jnp.broadcast_to(squares, (traits, 128))
        vals[6] = jnp.broadcast_to(ratio, (traits, 128))

    def turn(number):
        dir_ref[...] = ag[number].astype(F32) + vals[6][:, 0:1][None] * dir_ref[...]

    zero = jnp.zeros((traits, 1), F32)
    total, _ = sum_for_owner(0, lambda piece: dir_ref[piece] + drecv[piece], zero, True)
    search = total / noise_var + jnp.sqrt(ridge) * nco[...]
    search_ref[...] = search
    share(0, search, zero)
    swap_res.wait_recv()
    swap_geno.wait_recv()
    image_of(0, True)
    dir_ref[...] = jnp.zeros_like(dir_ref)

    def iterate(number, carry):
        own, pair = img[0], img[1]
        own_low = own.astype(BF16)
        pair_low = pair.astype(BF16)
        bend = jnp.sum(own * own_low.astype(F32), axis=1, keepdims=True)
        bend += jnp.sum(pair * pair_low.astype(F32), axis=1, keepdims=True)

        def part_of(piece):
            part = lax.dot_general(own_low, xh[0, piece], NN, preferred_element_type=F32)
            return part + lax.dot_general(pair_low, xh[1, piece], NN, preferred_element_type=F32)

        def meanwhile():
            turn(number - 1)

        total, bend = sum_for_owner(number, part_of, bend, False, meanwhile)
        step = vals[3][:, 0:1] / (bend / noise_var + ridge * vals[5][:, 0:1])
        applied = total / noise_var + ridge * dir_ref[r]
        search = search_ref[...] - step * applied
        search_ref[...] = search
        share(number, search, step)
        image_of(number, False)
        return carry

    lax.fori_loop(1, ITERS, iterate, 0)
    turn(ITERS - 1)

    swap_acc = to_pair(acc, c_recv, 3)
    swap_dir = to_pair(dir_ref, d_recv, 4)
    own, pair = img[0], img[1]
    squares = vals[5][:, 0:1]
    guess = vals[4][:, 0:1]
    left_own = pres[0] - fitted[0] - guess * own
    left_pair = pres[1] - fitted[1] - guess * pair

    def both(one, two):
        return jnp.sum(one, axis=1, keepdims=True) + jnp.sum(two, axis=1, keepdims=True)

    fin[z] = to_row(
        [
            both(own * own.astype(BF16).astype(F32), pair * pair.astype(BF16).astype(F32)),
            both(left_own * left_own, left_pair * left_pair),
            both(left_own * own, left_pair * pair),
            both(own * own, pair * pair),
        ]
    )
    half_way = chips // 2
    for offset in sorted(range(1, chips), key=lambda o: -min(o, chips - o)):
        pltpu.make_async_remote_copy(
            src_ref=fin.at[z],
            dst_ref=fin.at[z],
            send_sem=pair_send.at[5],
            recv_sem=pair_recv.at[5],
            device_id=chip(offset if offset <= half_way else offset - chips),
            device_id_type=MESH,
        ).start()
    swap_acc.start()
    swap_dir.start()
    present = jnp.int32(0)
    for device in range(chips * CORES):
        present += s_counts[device]
    others = fin.at[pl.ds(0, chips - 1)]
    pltpu.make_async_copy(others, others, pair_recv.at[5]).wait()
    line = fin[0]
    for place in range(1, chips):
        line += fin[place]
    norm_now = vals[3][:, 0:1]
    step = norm_now / (to_column(line, 0) / noise_var + ridge * squares)
    shift = step - guess
    left = to_column(line, 1) - 2.0 * shift * to_column(line, 2) + shift * shift * to_column(line, 3)
    scale = (present.astype(F32) + PRIOR_DOF) * vals[2][:, 0:1]
    sigma_out[...] = to_row([(left + PRIOR_DOF * PRIOR_SCALE) / scale])
    resid_out[...] = pres[0] - (fitted[0] + step * own)

    def put(start, place, steps, directions):
        for piece in range(NEAR):
            columns = slice(piece * width, (piece + 1) * width)
            new = steps[piece] + step * directions[piece]
            at = pl.multiple_of(start + piece * width, width)
            coef_out[:, pl.ds(at, width)] = jnp.where(first, new, cf[place, :, columns])
            at = pl.multiple_of(CORES * half + start + piece * width, width)
            coef_out[:, pl.ds(at, width)] = jnp.where(first, cf[place + 2, :, columns], new)

    put(mine, 0, acc, dir_ref)
    swap_acc.wait_recv()
    swap_dir.wait_recv()
    put(other, 1, c_recv, d_recv)

    for swap in (swap_sum, swap_res, swap_geno, swap_acc, swap_dir):
        swap.wait_send()
    pltpu.make_async_copy(others, others, pair_send.at[5]).wait()

    def sent(ref, stage, number):
        pltpu.make_async_copy(ref, ref, st_send.at[number, stage]).wait()

    def drain(number, carry):
        sent(rs_recv.at[number], 0, number)
        sent(cv_recv.at[number], 1, number)
        for stage in (2, 8, 10):
            sent(mid.at[number, 0], stage, number)
            sent(mcv.at[number, 0], stage + 1, number)
        sent(agn.at[number, pl.ds(0, NEAR - 1)], 5, number)
        sent(img_recv.at[number], 6, number)
        sent(dd_recv.at[number], 7, number)
        for stage, offsets in enumerate(TAKES):
            sent(ag.at[number, pl.ds(0, len(offsets) - (0 in offsets))], 12 + stage, number)
        return carry

    lax.fori_loop(0, ITERS, drain, 0)


def update(geno, resid, npeople, ncoef, coef, block, prior, sigma, gamma, counts):
    rows, batch = geno.shape
    traits = resid.shape[0]
    devices = lax.axis_size(AXIS)
    chips = devices // CORES
    half = batch // CORES
    width = half // NEAR
    groups = chips // NEAR
    outside = pl.BlockSpec(memory_space=pltpu.HBM)
    inside = pl.BlockSpec(memory_space=pltpu.VMEM)
    block16 = (NEAR, traits, width)
    return pl.pallas_call(
        functools.partial(kernel, chips),
        name="gibbs",
        out_shape=(
            jax.ShapeDtypeStruct(coef.shape, F32),
            jax.ShapeDtypeStruct((traits, rows), F32),
            jax.ShapeDtypeStruct((1, 128), F32),
        ),
        in_specs=[outside] * 10,
        out_specs=(inside,) * 3,
        scratch_shapes=[
            pltpu.VMEM((2, NEAR, rows, width), BF16),
            pltpu.VMEM((NEAR, rows, width), BF16),
            pltpu.VMEM((4, traits, half), F32),
            pltpu.VMEM((traits, rows), F32),
            pltpu.VMEM((traits, rows), F32),
            pltpu.VMEM((traits, width), F32),
            pltpu.SMEM((1,), jnp.int32),
            pltpu.SMEM((traits,), F32),
            pltpu.SMEM((traits,), F32),
            pltpu.SMEM((traits,), F32),
            pltpu.SMEM((devices,), jnp.int32),
            pltpu.VMEM((2, traits, rows), F32),
            pltpu.VMEM(block16, F32),
            pltpu.VMEM(block16, F32),
            pltpu.VMEM((traits, width), F32),
            pltpu.VMEM((ITERS, *block16), jnp.int16),
            pltpu.VMEM((ITERS, 7, traits, width), jnp.int16),
            pltpu.VMEM((ITERS, NEAR, 1, 128), F32),
            pltpu.VMEM((ITERS, 8, 1, 128), F32),
            pltpu.VMEM((ITERS, groups, traits, width), jnp.int16),
            pltpu.VMEM((ITERS, groups, 1, 128), F32),
            pltpu.VMEM((ITERS, *block16), BF16),
            pltpu.VMEM((ITERS, NEAR, 1, 128), F32),
            pltpu.VMEM((traits, width), F32),
            pltpu.VMEM(block16, F32),
            pltpu.VMEM(block16, F32),
            pltpu.VMEM((ITERS, 2, traits, rows), F32),
            pltpu.VMEM((ITERS, 2, traits, rows), F32),
            pltpu.VMEM((ITERS, 1, 128), F32),
            pltpu.VMEM((ITERS, 1, 128), F32),
            pltpu.VMEM((2, traits, rows), F32),
            pltpu.VMEM((2, traits, rows), F32),
            pltpu.VMEM((chips, 1, 128), F32),
            pltpu.VMEM(block16, F32),
            pltpu.VMEM(block16, F32),
            pltpu.VMEM((7, traits, 128), F32),
            pltpu.SemaphoreType.DMA((23,)),
            pltpu.SemaphoreType.DMA((5,)),
            pltpu.SemaphoreType.DMA((6,)),
            pltpu.SemaphoreType.DMA((6,)),
            pltpu.SemaphoreType.DMA((ITERS, 15)),
            pltpu.SemaphoreType.DMA((ITERS, 15)),
        ],
        compiler_params=pltpu.CompilerParams(
            collective_id=0, has_side_effects=True, vmem_limit_bytes=64 * 1000 * 1000


        ),
    )(geno, resid, npeople, ncoef, coef, block, prior, sigma, gamma, counts)


def per_device(geno, resid, npeople, ncoef, coef, block, prior, sigma, gamma, counts):
    coef_new, resid_new, sigma_line = update(
        geno, resid, npeople, ncoef, coef, block, prior, sigma, gamma, counts
    )
    return coef_new, resid_new, sigma_line[0, : resid.shape[0]]


def solution(mesh):
    return jax.shard_map(
        per_device,
        mesh=mesh,
        in_specs=(
            P(("trait", "ppl"), None),
            P("trait", "ppl"),
            P("trait", "ppl"),
            P("trait", None),
            P("trait", None),
            P("trait"),
            P("trait"),
            P("trait"),
            P("trait"),
            P("trait"),
        ),
        out_specs=(P("trait", None), P("trait", "ppl"), P("trait")),
        check_vma=False,
    )
```

```python
import functools

import jax
import jax.numpy as jnp
from jax import lax
from jax.experimental import pallas as pl
from jax.experimental.pallas import tpu as pltpu
from jax.sharding import PartitionSpec as P

ITERS = 4
PRIOR_DOF = 4.0
PRIOR_SCALE = 0.5
AXIS = "ppl"
CORES = 2
NEAR = 8
MESH = pl.DeviceIdType.MESH
F32 = jnp.float32
BF16 = jnp.bfloat16
NT = (((1,), (1,)), ((), ()))
NN = (((1,), (0,)), ((), ()))
CODES = 32000.0
FULL = (3, -3, 2, -2, 1, -1)
ENDS = (NEAR // 2, -(NEAR // 2))
SENDS = ((NEAR // 2, 3, -3), (2, -2), (1, -1), (0,))
TAKES = ((0, 1, -1), (2, -2), (3, -3, NEAR // 2))
TAKE_OF = {sign * abs(o): 12 + i for i, offsets in enumerate(TAKES) for o in offsets for sign in (1, -1)}


def kernel(
    chips,
    geno,
    resid,
    npeople,
    ncoef,
    coef,
    block,
    prior,
    sigma,
    gamma,
    counts,
    coef_out,
    resid_out,
    sigma_out,
    xh,
    xo,
    cf,
    res,
    npl,
    nco,
    s_block,
    s_prior,
    s_sigma,
    s_gamma,
    s_counts,
    pres,
    dsend,
    drecv,
    rs_own,
    rs_send,
    rs_recv,
    cv_send,
    cv_recv,
    mid,
    mcv,
    ag,
    agn,
    search_ref,
    dir_ref,
    acc,
    img_send,
    img_recv,
    dd_send,
    dd_recv,
    img,
    fitted,
    fin,
    c_recv,
    d_recv,
    vals,
    load_sem,
    small_sem,
    pair_send,
    pair_recv,
    st_send,
    st_recv,
):
    traits, rows = res.shape
    width = xo.shape[2]
    half = NEAR * width
    groups = chips // NEAR
    top = traits // 2
    me = lax.axis_index(AXIS)
    z = me // CORES
    k = lax.rem(me, CORES)
    g = z // NEAR
    r = lax.rem(z, NEAR)
    partner = {AXIS: z * CORES + (1 - k)}

    def chip(offset):
        return {AXIS: lax.rem(z + offset + chips, chips) * CORES + k}

    def piece_at(offset):
        return lax.rem(r + offset + NEAR, NEAR)

    mine = pl.multiple_of(k * half, half)
    other = pl.multiple_of((1 - k) * half, half)
    own_col = pl.multiple_of(k * half + r * width, width)
    loads = [
        pltpu.make_async_copy(coef.at[:, pl.ds(mine, half)], cf.at[0], load_sem.at[0]),
        pltpu.make_async_copy(coef.at[:, pl.ds(other, half)], cf.at[1], load_sem.at[1]),
        pltpu.make_async_copy(coef.at[:, pl.ds(2 * half + mine, half)], cf.at[2], load_sem.at[2]),
        pltpu.make_async_copy(coef.at[:, pl.ds(2 * half + other, half)], cf.at[3], load_sem.at[3]),
        pltpu.make_async_copy(resid, res, load_sem.at[4]),
        pltpu.make_async_copy(npeople, npl, load_sem.at[5]),
        pltpu.make_async_copy(ncoef.at[:, pl.ds(own_col, width)], nco, load_sem.at[6]),
    ]
    for piece in range(NEAR):
        at = pl.multiple_of(mine + piece * width, width)
        loads.append(
            pltpu.make_async_copy(geno.at[:, pl.ds(at, width)], xh.at[0, piece], load_sem.at[7 + piece])
        )
        at = pl.multiple_of(other + piece * width, width)
        loads.append(
            pltpu.make_async_copy(geno.at[:, pl.ds(at, width)], xo.at[piece], load_sem.at[15 + piece])
        )
    smalls = [
        pltpu.make_async_copy(block, s_block, small_sem.at[0]),
        pltpu.make_async_copy(prior, s_prior, small_sem.at[1]),
        pltpu.make_async_copy(sigma, s_sigma, small_sem.at[2]),
        pltpu.make_async_copy(gamma, s_gamma, small_sem.at[3]),
        pltpu.make_async_copy(counts, s_counts, small_sem.at[4]),
    ]
    for copy in smalls + loads:
        copy.start()
    barrier = pltpu.get_barrier_semaphore()
    for target in (*[chip(offset) for offset in (*ENDS, *FULL)], partner):
        pl.semaphore_signal(barrier, inc=1, device_id=target, device_id_type=MESH)
    for copy in smalls:
        copy.wait()

    row_id = lax.broadcasted_iota(jnp.int32, (traits, 128), 0)
    lane_id = lax.broadcasted_iota(jnp.int32, (traits, 128), 1)

    def to_row(columns):
        total = jnp.zeros((traits, 128), F32)
        for place, column in enumerate(columns):
            total += jnp.where(lane_id == row_id + place * traits, column, 0.0)
        return jnp.sum(total, axis=0, keepdims=True)

    def to_column(line, place):
        return jnp.sum(
            jnp.where(lane_id == row_id + place * traits, line, 0.0), axis=1, keepdims=True
        )

    def column_of(ref):
        column = jnp.zeros((traits, 128), F32)
        for trait in range(traits):
            column = jnp.where(row_id == trait, ref[trait], column)
        return column

    vals[0] = column_of(s_sigma)
    vals[1] = column_of(s_prior)
    vals[2] = column_of(s_gamma)
    noise_var = vals[0][:, 0:1]
    ridge = vals[1][:, 0:1]
    slot = lax.broadcasted_iota(jnp.int32, (traits, rows), 1)
    mask_own = (slot < s_counts[me]).astype(F32)
    mask_pair = (slot < s_counts[z * CORES + (1 - k)]).astype(F32)

    def coded(values):
        largest = jnp.maximum(jnp.max(jnp.abs(values), axis=1, keepdims=True), 1e-30)
        codes = jnp.round(values * (CODES / largest)).astype(jnp.int32).astype(jnp.int16)
        return codes, largest * (1.0 / CODES)

    def decoded(codes, unit):
        return codes.astype(jnp.int32).astype(F32) * unit

    few = len(loads) - 2 * NEAR
    for copy in loads[:few]:
        copy.wait()
    first = s_block[0] == 0
    old_mine = jnp.where(first, cf[0], cf[2]).astype(BF16)
    old_other = jnp.where(first, cf[1], cf[3]).astype(BF16)
    fitted_old = jnp.zeros((traits, rows), F32)
    for piece in range(NEAR):
        columns = slice(piece * width, (piece + 1) * width)
        loads[few + 2 * piece].wait()
        loads[few + 2 * piece + 1].wait()
        fitted_old += lax.dot_general(old_mine[:, columns], xh[0, piece], NT, preferred_element_type=F32)
        fitted_old += lax.dot_general(old_other[:, columns], xo[piece], NT, preferred_element_type=F32)
    partial_res = mask_own * (res[...] + fitted_old)
    pres[0] = partial_res
    target = (mask_own * (partial_res + jnp.sqrt(noise_var) * npl[...])).astype(BF16)
    for piece in range(NEAR):
        dsend[piece] = lax.dot_general(target, xo[piece], NN, preferred_element_type=F32)

    pl.semaphore_wait(barrier, len(ENDS) + len(FULL) + 1)

    def to_pair(src, dst, index):
        return pltpu.make_async_remote_copy(
            src_ref=src,
            dst_ref=dst,
            send_sem=pair_send.at[index],
            recv_sem=pair_recv.at[index],
            device_id=partner,
            device_id_type=MESH,
        )

    swap_sum = to_pair(dsend, drecv, 0)
    swap_res = to_pair(pres.at[0], pres.at[1], 1)
    swap_geno = to_pair(xo, xh.at[1], 2)
    swap_sum.start()
    swap_res.start()
    swap_geno.start()
    for piece in range(NEAR):
        dir_ref[piece] = lax.dot_general(target, xh[0, piece], NN, preferred_element_type=F32)
    fitted[...] = jnp.zeros_like(fitted)
    acc[...] = jnp.zeros_like(acc)
    swap_sum.wait_recv()

    def send(src, dst, stage, number, target):
        pltpu.make_async_remote_copy(
            src_ref=src,
            dst_ref=dst,
            send_sem=st_send.at[number, stage],
            recv_sem=st_recv.at[number, stage],
            device_id=target,
            device_id_type=MESH,
        ).start()

    def arrived(ref, stage, number):
        pltpu.make_async_copy(ref, ref, st_recv.at[number, stage]).wait()

    def sum_for_owner(number, part_of, column, relay, meanwhile=lambda: None):
        for offsets in SENDS:
            pieces = [piece_at(offset) for offset in offsets]
            for offset, piece, part in zip(offsets, pieces, [part_of(piece) for piece in pieces]):
                if offset == 0:
                    rs_own[...] = part
                    continue
                rs_send[number, piece], unit = coded(part)
                cv_send[number, piece] = to_row([column, unit])
            for offset, piece in zip(offsets, pieces):
                line = cv_send.at[number, piece]
                codes = rs_send.at[number, piece]
                if offset == ENDS[0]:
                    for place, end in enumerate(ENDS):
                        band = pl.ds(place * top, top)
                        send(line, cv_recv.at[number, 6 + place], 1, number, chip(end))
                        send(
                            codes.at[band], rs_recv.at[number, 6, band], 0, number, chip(end)
                        )
                elif offset:
                    slot_id = FULL.index(offset)
                    send(line, cv_recv.at[number, slot_id], 1, number, chip(offset))
                    send(codes, rs_recv.at[number, slot_id], 0, number, chip(offset))
        meanwhile()
        arrived(cv_recv.at[number], 1, number)
        sums = to_row([column])
        for slot_id in range(7):
            sums += cv_recv[number, slot_id]
        sums = to_column(sums, 0)
        upper = lax.broadcasted_iota(jnp.int32, (traits, 1), 0) < top
        arrived(rs_recv.at[number], 0, number)
        total = rs_own[...]
        for slot_id in range(6):
            total += decoded(rs_recv[number, slot_id], to_column(cv_recv[number, slot_id], 1))
        unit = jnp.where(upper, to_column(cv_recv[number, 6], 1), to_column(cv_recv[number, 7], 1))
        total += decoded(rs_recv[number, 6], unit)
        mid[number, g], unit = coded(total)
        mcv[number, g] = to_row([sums, unit])

        def pass_on(group, offset, stage):
            send(mcv.at[number, group], mcv.at[number, group], stage + 1, number, chip(offset))
            send(mid.at[number, group], mid.at[number, group], stage, number, chip(offset))

        if not relay:
            pass_on(g, 2 * NEAR, 10)
        pass_on(g, NEAR, 2)
        pass_on(g, -NEAR, 8)
        arrived(mcv.at[number, 0], 9, number)
        arrived(mid.at[number, 0], 8, number)
        if relay:
            pass_on(lax.rem(g + 1, groups), -NEAR, 10)
        arrived(mcv.at[number, 0], 3, number)
        arrived(mid.at[number, 0], 2, number)
        arrived(mcv.at[number, 0], 11, number)
        arrived(mid.at[number, 0], 10, number)
        sums = mcv[number, 0]
        total = decoded(mid[number, 0], to_column(sums, 1))
        for group in range(1, groups):
            line = mcv[number, group]
            sums += line
            total += decoded(mid[number, group], to_column(line, 1))
        return total, to_column(sums, 0)

    def share(number, search, step):
        ag[number, r] = search.astype(BF16)
        agn[number, r] = to_row([jnp.sum(search * search, axis=1, keepdims=True), step])
        for place, end in enumerate(ENDS):
            band = pl.ds(place * top, top)
            send(ag.at[number, r, band], ag.at[number, r, band], TAKE_OF[end], number, chip(end))
            if place == 0:
                send(agn.at[number, r], agn.at[number, r], 5, number, chip(end))
        for offset in FULL:
            send(ag.at[number, r], ag.at[number, r], TAKE_OF[offset], number, chip(offset))
            send(agn.at[number, r], agn.at[number, r], 5, number, chip(offset))

    def image_of(number, fresh):
        own = jnp.zeros((traits, rows), F32)
        pair = jnp.zeros((traits, rows), F32)
        squares = jnp.zeros((traits, 1), F32)
        cross = jnp.zeros((traits, 1), F32)
        for stage, offsets in enumerate(TAKES):
            arrived(ag.at[number, pl.ds(0, len(offsets) - (0 in offsets))], 12 + stage, number)
            for offset in offsets:
                piece = piece_at(offset)
                low = ag[number, piece]
                own += lax.dot_general(low, xh[0, piece], NT, preferred_element_type=F32)
                pair += lax.dot_general(low, xh[1, piece], NT, preferred_element_type=F32)
                wide = low.astype(F32)
                squares += jnp.sum(wide * wide, axis=1, keepdims=True)
                if not fresh:
                    cross += jnp.sum(wide * dir_ref[piece], axis=1, keepdims=True)
        img_send[number, 0] = pair
        img_send[number, 1] = own
        send(img_send.at[number], img_recv.at[number], 6, number, partner)
        arrived(agn.at[number, pl.ds(0, NEAR - 1)], 5, number)
        line = agn[number, 0]
        for place in range(1, NEAR):
            line += agn[number, place]
        dd_send[number] = to_row([to_column(line, 0), squares, cross])
        send(dd_send.at[number], dd_recv.at[number], 7, number, partner)
        step = to_column(agn[number, 0], 1)
        if not fresh:
            fitted[...] += step[None] * img[...]
            acc[...] += step[None] * dir_ref[...]
        arrived(dd_recv.at[number], 7, number)
        line = dd_send[number] + dd_recv[number]
        norm = to_column(line, 0)
        squares = to_column(line, 1)
        arrived(img_recv.at[number], 6, number)
        own = mask_own * (own + img_recv[number, 0])
        pair = mask_pair * (pair + img_recv[number, 1])
        if fresh:
            ratio = jnp.zeros((traits, 1), F32)
        else:
            ratio = norm / vals[3][:, 0:1]
            own += ratio * img[0]
            pair += ratio * img[1]
            squares += ratio * (2.0 * to_column(line, 2) + ratio * vals[5][:, 0:1])
        img[0] = own
        img[1] = pair
        vals[3] = jnp.broadcast_to(norm, (traits, 128))
        vals[4] = jnp.broadcast_to(step, (traits, 128))
        vals[5] = jnp.broadcast_to(squares, (traits, 128))
        vals[6] = jnp.broadcast_to(ratio, (traits, 128))

    def turn(number):
        dir_ref[...] = ag[number].astype(F32) + vals[6][:, 0:1][None] * dir_ref[...]

    zero = jnp.zeros((traits, 1), F32)
    total, _ = sum_for_owner(0, lambda piece: dir_ref[piece] + drecv[piece], zero, True)
    search = total / noise_var + jnp.sqrt(ridge) * nco[...]
    search_ref[...] = search
    share(0, search, zero)
    swap_res.wait_recv()
    swap_geno.wait_recv()
    image_of(0, True)
    dir_ref[...] = jnp.zeros_like(dir_ref)

    def iterate(number, carry):
        own, pair = img[0], img[1]
        own_low = own.astype(BF16)
        pair_low = pair.astype(BF16)
        bend = jnp.sum(own * own_low.astype(F32), axis=1, keepdims=True)
        bend += jnp.sum(pair * pair_low.astype(F32), axis=1, keepdims=True)

        def part_of(piece):
            part = lax.dot_general(own_low, xh[0, piece], NN, preferred_element_type=F32)
            return part + lax.dot_general(pair_low, xh[1, piece], NN, preferred_element_type=F32)

        def meanwhile():
            turn(number - 1)

        total, bend = sum_for_owner(number, part_of, bend, False, meanwhile)
        step = vals[3][:, 0:1] / (bend / noise_var + ridge * vals[5][:, 0:1])
        applied = total / noise_var + ridge * dir_ref[r]
        search = search_ref[...] - step * applied
        search_ref[...] = search
        share(number, search, step)
        image_of(number, False)
        return carry

    lax.fori_loop(1, ITERS, iterate, 0)
    turn(ITERS - 1)

    swap_acc = to_pair(acc, c_recv, 3)
    swap_dir = to_pair(dir_ref, d_recv, 4)
    own, pair = img[0], img[1]
    squares = vals[5][:, 0:1]
    guess = vals[4][:, 0:1]
    left_own = pres[0] - fitted[0] - guess * own
    left_pair = pres[1] - fitted[1] - guess * pair

    def both(one, two):
        return jnp.sum(one, axis=1, keepdims=True) + jnp.sum(two, axis=1, keepdims=True)

    fin[z] = to_row(
        [
            both(own * own.astype(BF16).astype(F32), pair * pair.astype(BF16).astype(F32)),
            both(left_own * left_own, left_pair * left_pair),
            both(left_own * own, left_pair * pair),
            both(own * own, pair * pair),
        ]
    )
    half_way = chips // 2
    for offset in sorted(range(1, chips), key=lambda o: -min(o, chips - o)):
        pltpu.make_async_remote_copy(
            src_ref=fin.at[z],
            dst_ref=fin.at[z],
            send_sem=pair_send.at[5],
            recv_sem=pair_recv.at[5],
            device_id=chip(offset if offset <= half_way else offset - chips),
            device_id_type=MESH,
        ).start()
    swap_acc.start()
    swap_dir.start()
    present = jnp.int32(0)
    for device in range(chips * CORES):
        present += s_counts[device]
    others = fin.at[pl.ds(0, chips - 1)]
    pltpu.make_async_copy(others, others, pair_recv.at[5]).wait()
    line = fin[0]
    for place in range(1, chips):
        line += fin[place]
    norm_now = vals[3][:, 0:1]
    step = norm_now / (to_column(line, 0) / noise_var + ridge * squares)
    shift = step - guess
    left = to_column(line, 1) - 2.0 * shift * to_column(line, 2) + shift * shift * to_column(line, 3)
    scale = (present.astype(F32) + PRIOR_DOF) * vals[2][:, 0:1]
    sigma_out[...] = to_row([(left + PRIOR_DOF * PRIOR_SCALE) / scale])
    resid_out[...] = pres[0] - (fitted[0] + step * own)

    def put(start, place, steps, directions):
        for piece in range(NEAR):
            columns = slice(piece * width, (piece + 1) * width)
            new = steps[piece] + step * directions[piece]
            at = pl.multiple_of(start + piece * width, width)
            coef_out[:, pl.ds(at, width)] = jnp.where(first, new, cf[place, :, columns])
            at = pl.multiple_of(CORES * half + start + piece * width, width)
            coef_out[:, pl.ds(at, width)] = jnp.where(first, cf[place + 2, :, columns], new)

    put(mine, 0, acc, dir_ref)
    swap_acc.wait_recv()
    swap_dir.wait_recv()
    put(other, 1, c_recv, d_recv)

    for swap in (swap_sum, swap_res, swap_geno, swap_acc, swap_dir):
        swap.wait_send()
    pltpu.make_async_copy(others, others, pair_send.at[5]).wait()

    def sent(ref, stage, number):
        pltpu.make_async_copy(ref, ref, st_send.at[number, stage]).wait()

    def drain(number, carry):
        sent(rs_recv.at[number], 0, number)
        sent(cv_recv.at[number], 1, number)
        for stage in (2, 8, 10):
            sent(mid.at[number, 0], stage, number)
            sent(mcv.at[number, 0], stage + 1, number)
        sent(agn.at[number, pl.ds(0, NEAR - 1)], 5, number)
        sent(img_recv.at[number], 6, number)
        sent(dd_recv.at[number], 7, number)
        for stage, offsets in enumerate(TAKES):
            sent(ag.at[number, pl.ds(0, len(offsets) - (0 in offsets))], 12 + stage, number)
        return carry

    lax.fori_loop(0, ITERS, drain, 0)


def loose(array):
    return pltpu.with_memory_space_constraint(array, pltpu.HBM)


def update(geno, resid, npeople, ncoef, coef, block, prior, sigma, gamma, counts):
    rows, batch = geno.shape
    traits = resid.shape[0]
    devices = lax.axis_size(AXIS)
    chips = devices // CORES
    half = batch // CORES
    width = half // NEAR
    groups = chips // NEAR
    outside = pl.BlockSpec(memory_space=pltpu.HBM)
    inside = pl.BlockSpec(memory_space=pltpu.VMEM)
    block16 = (NEAR, traits, width)
    return pl.pallas_call(
        functools.partial(kernel, chips),
        name="gibbs",
        out_shape=(
            jax.ShapeDtypeStruct(coef.shape, F32),
            jax.ShapeDtypeStruct((traits, rows), F32),
            jax.ShapeDtypeStruct((1, 128), F32),
        ),
        in_specs=[outside] * 10,
        out_specs=(inside,) * 3,
        scratch_shapes=[
            pltpu.VMEM((2, NEAR, rows, width), BF16),
            pltpu.VMEM((NEAR, rows, width), BF16),
            pltpu.VMEM((4, traits, half), F32),
            pltpu.VMEM((traits, rows), F32),
            pltpu.VMEM((traits, rows), F32),
            pltpu.VMEM((traits, width), F32),
            pltpu.SMEM((1,), jnp.int32),
            pltpu.SMEM((traits,), F32),
            pltpu.SMEM((traits,), F32),
            pltpu.SMEM((traits,), F32),
            pltpu.SMEM((devices,), jnp.int32),
            pltpu.VMEM((2, traits, rows), F32),
            pltpu.VMEM(block16, F32),
            pltpu.VMEM(block16, F32),
            pltpu.VMEM((traits, width), F32),
            pltpu.VMEM((ITERS, *block16), jnp.int16),
            pltpu.VMEM((ITERS, 7, traits, width), jnp.int16),
            pltpu.VMEM((ITERS, NEAR, 1, 128), F32),
            pltpu.VMEM((ITERS, 8, 1, 128), F32),
            pltpu.VMEM((ITERS, groups, traits, width), jnp.int16),
            pltpu.VMEM((ITERS, groups, 1, 128), F32),
            pltpu.VMEM((ITERS, *block16), BF16),
            pltpu.VMEM((ITERS, NEAR, 1, 128), F32),
            pltpu.VMEM((traits, width), F32),
            pltpu.VMEM(block16, F32),
            pltpu.VMEM(block16, F32),
            pltpu.VMEM((ITERS, 2, traits, rows), F32),
            pltpu.VMEM((ITERS, 2, traits, rows), F32),
            pltpu.VMEM((ITERS, 1, 128), F32),
            pltpu.VMEM((ITERS, 1, 128), F32),
            pltpu.VMEM((2, traits, rows), F32),
            pltpu.VMEM((2, traits, rows), F32),
            pltpu.VMEM((chips, 1, 128), F32),
            pltpu.VMEM(block16, F32),
            pltpu.VMEM(block16, F32),
            pltpu.VMEM((7, traits, 128), F32),
            pltpu.SemaphoreType.DMA((23,)),
            pltpu.SemaphoreType.DMA((5,)),
            pltpu.SemaphoreType.DMA((6,)),
            pltpu.SemaphoreType.DMA((6,)),
            pltpu.SemaphoreType.DMA((ITERS, 15)),
            pltpu.SemaphoreType.DMA((ITERS, 15)),
        ],
        compiler_params=pltpu.CompilerParams(
            collective_id=0, has_side_effects=True, vmem_limit_bytes=40 * 1000 * 1000


        ),
    )(
        *map(loose, (geno, resid, npeople, ncoef, coef)),
        block,
        *map(loose, (prior, sigma, gamma, counts)),
    )


def per_device(geno, resid, npeople, ncoef, coef, block, prior, sigma, gamma, counts):
    coef_new, resid_new, sigma_line = update(
        geno, resid, npeople, ncoef, coef, block, prior, sigma, gamma, counts
    )
    return coef_new, resid_new, sigma_line[0, : resid.shape[0]]


def solution(mesh):
    return jax.shard_map(
        per_device,
        mesh=mesh,
        in_specs=(
            P(("trait", "ppl"), None),
            P("trait", "ppl"),
            P("trait", "ppl"),
            P("trait", None),
            P("trait", None),
            P("trait"),
            P("trait"),
            P("trait"),
            P("trait"),
            P("trait"),
        ),
        out_specs=(P("trait", None), P("trait", "ppl"), P("trait")),
        check_vma=False,
    )
```

```python
import functools

import jax
import jax.numpy as jnp
from jax import lax
from jax.experimental import pallas as pl
from jax.experimental.pallas import tpu as pltpu
from jax.sharding import PartitionSpec as P

ITERS = 4
PRIOR_DOF = 4.0
PRIOR_SCALE = 0.5
AXIS = "ppl"
CORES = 2
NEAR = 8
MESH = pl.DeviceIdType.MESH
F32 = jnp.float32
BF16 = jnp.bfloat16
NT = (((1,), (1,)), ((), ()))
NN = (((1,), (0,)), ((), ()))
CODES = 32000.0
FULL = (3, -3, 2, -2, 1, -1)
ENDS = (NEAR // 2, -(NEAR // 2))
SENDS = ((NEAR // 2, 3, -3), (2, -2), (1, -1), (0,))
TAKES = ((0, 1, -1), (2, -2), (3, -3, NEAR // 2))
TAKE_OF = {sign * abs(o): 12 + i for i, offsets in enumerate(TAKES) for o in offsets for sign in (1, -1)}


def kernel(
    chips,
    geno,
    resid,
    npeople,
    ncoef,
    coef,
    block,
    prior,
    sigma,
    gamma,
    counts,
    coef_out,
    resid_out,
    sigma_out,
    xh,
    xo,
    cf,
    res,
    npl,
    nco,
    s_block,
    s_prior,
    s_sigma,
    s_gamma,
    s_counts,
    pres,
    dsend,
    drecv,
    rs_own,
    rs_send,
    rs_recv,
    cv_send,
    cv_recv,
    mid,
    mcv,
    ag,
    agn,
    search_ref,
    dir_ref,
    acc,
    img_send,
    img_recv,
    dd_send,
    dd_recv,
    img,
    fitted,
    fin,
    c_recv,
    d_recv,
    vals,
    load_sem,
    small_sem,
    pair_send,
    pair_recv,
    st_send,
    st_recv,
):
    traits, rows = res.shape
    width = xo.shape[2]
    half = NEAR * width
    groups = chips // NEAR
    top = traits // 2
    me = lax.axis_index(AXIS)
    z = me // CORES
    k = lax.rem(me, CORES)
    g = z // NEAR
    r = lax.rem(z, NEAR)
    partner = {AXIS: z * CORES + (1 - k)}

    near = {o: {AXIS: lax.rem(z + o + chips, chips) * CORES + k} for o in (*ENDS, *FULL, NEAR, -NEAR)}

    def chip(offset):
        return near.get(offset) or {AXIS: lax.rem(z + offset + chips, chips) * CORES + k}

    def piece_at(offset):
        return lax.rem(r + offset + NEAR, NEAR)

    mine = pl.multiple_of(k * half, half)
    other = pl.multiple_of((1 - k) * half, half)
    own_col = pl.multiple_of(k * half + r * width, width)
    loads = [
        pltpu.make_async_copy(coef.at[:, pl.ds(mine, half)], cf.at[0], load_sem.at[0]),
        pltpu.make_async_copy(coef.at[:, pl.ds(other, half)], cf.at[1], load_sem.at[1]),
        pltpu.make_async_copy(coef.at[:, pl.ds(2 * half + mine, half)], cf.at[2], load_sem.at[2]),
        pltpu.make_async_copy(coef.at[:, pl.ds(2 * half + other, half)], cf.at[3], load_sem.at[3]),
        pltpu.make_async_copy(resid, res, load_sem.at[4]),
        pltpu.make_async_copy(npeople, npl, load_sem.at[5]),
        pltpu.make_async_copy(ncoef.at[:, pl.ds(own_col, width)], nco, load_sem.at[6]),
    ]
    for piece in range(NEAR):
        at = pl.multiple_of(mine + piece * width, width)
        loads.append(
            pltpu.make_async_copy(geno.at[:, pl.ds(at, width)], xh.at[0, piece], load_sem.at[7 + piece])
        )
        at = pl.multiple_of(other + piece * width, width)
        loads.append(
            pltpu.make_async_copy(geno.at[:, pl.ds(at, width)], xo.at[piece], load_sem.at[15 + piece])
        )
    smalls = [
        pltpu.make_async_copy(block, s_block, small_sem.at[0]),
        pltpu.make_async_copy(prior, s_prior, small_sem.at[1]),
        pltpu.make_async_copy(sigma, s_sigma, small_sem.at[2]),
        pltpu.make_async_copy(gamma, s_gamma, small_sem.at[3]),
        pltpu.make_async_copy(counts, s_counts, small_sem.at[4]),
    ]
    for copy in smalls + loads:
        copy.start()
    barrier = pltpu.get_barrier_semaphore()
    for target in (*[chip(offset) for offset in (*ENDS, *FULL)], partner):
        pl.semaphore_signal(barrier, inc=1, device_id=target, device_id_type=MESH)
    for copy in smalls:
        copy.wait()

    row_id = lax.broadcasted_iota(jnp.int32, (traits, 128), 0)
    lane_id = lax.broadcasted_iota(jnp.int32, (traits, 128), 1)

    def to_row(columns):
        total = jnp.zeros((traits, 128), F32)
        for place, column in enumerate(columns):
            total += jnp.where(lane_id == row_id + place * traits, column, 0.0)
        return jnp.sum(total, axis=0, keepdims=True)

    def to_column(line, place):
        return jnp.sum(
            jnp.where(lane_id == row_id + place * traits, line, 0.0), axis=1, keepdims=True
        )

    def column_of(ref):
        column = jnp.zeros((traits, 128), F32)
        for trait in range(traits):
            column = jnp.where(row_id == trait, ref[trait], column)
        return column

    vals[0] = column_of(s_sigma)
    vals[1] = column_of(s_prior)
    vals[2] = column_of(s_gamma)
    noise_var = vals[0][:, 0:1]
    ridge = vals[1][:, 0:1]
    slot = lax.broadcasted_iota(jnp.int32, (traits, rows), 1)
    mask_own = (slot < s_counts[me]).astype(F32)
    mask_pair = (slot < s_counts[z * CORES + (1 - k)]).astype(F32)

    def coded(values):
        largest = jnp.maximum(jnp.max(jnp.abs(values), axis=1, keepdims=True), 1e-30)
        codes = jnp.round(values * (CODES / largest)).astype(jnp.int32).astype(jnp.int16)
        return codes, largest * (1.0 / CODES)

    def decoded(codes, unit):
        return codes.astype(jnp.int32).astype(F32) * unit

    for copy in loads:
        copy.wait()
    first = s_block[0] == 0
    old_mine = jnp.where(first, cf[0], cf[2]).astype(BF16)
    old_other = jnp.where(first, cf[1], cf[3]).astype(BF16)
    fitted_old = jnp.zeros((traits, rows), F32)
    for piece in range(NEAR):
        columns = slice(piece * width, (piece + 1) * width)
        fitted_old += lax.dot_general(old_mine[:, columns], xh[0, piece], NT, preferred_element_type=F32)
        fitted_old += lax.dot_general(old_other[:, columns], xo[piece], NT, preferred_element_type=F32)
    partial_res = mask_own * (res[...] + fitted_old)
    pres[0] = partial_res
    target = (mask_own * (partial_res + jnp.sqrt(noise_var) * npl[...])).astype(BF16)
    for piece in range(NEAR):
        dsend[piece] = lax.dot_general(target, xo[piece], NN, preferred_element_type=F32)

    pl.semaphore_wait(barrier, len(ENDS) + len(FULL) + 1)

    def to_pair(src, dst, index):
        return pltpu.make_async_remote_copy(
            src_ref=src,
            dst_ref=dst,
            send_sem=pair_send.at[index],
            recv_sem=pair_recv.at[index],
            device_id=partner,
            device_id_type=MESH,
        )

    swap_sum = to_pair(dsend, drecv, 0)
    swap_res = to_pair(pres.at[0], pres.at[1], 1)
    swap_geno = to_pair(xo, xh.at[1], 2)
    swap_sum.start()
    swap_res.start()
    swap_geno.start()
    for piece in range(NEAR):
        dir_ref[piece] = lax.dot_general(target, xh[0, piece], NN, preferred_element_type=F32)
    fitted[...] = jnp.zeros_like(fitted)
    acc[...] = jnp.zeros_like(acc)
    swap_sum.wait_recv()

    def send(src, dst, stage, number, target):
        pltpu.make_async_remote_copy(
            src_ref=src,
            dst_ref=dst,
            send_sem=st_send.at[number, stage],
            recv_sem=st_recv.at[number, stage],
            device_id=target,
            device_id_type=MESH,
        ).start()

    def arrived(ref, stage, number):
        pltpu.make_async_copy(ref, ref, st_recv.at[number, stage]).wait()

    def sum_for_owner(number, part_of, column, relay, meanwhile=lambda: None):
        for offsets in SENDS:
            pieces = [piece_at(offset) for offset in offsets]
            for offset, piece, part in zip(offsets, pieces, [part_of(piece) for piece in pieces]):
                if offset == 0:
                    rs_own[...] = part
                    continue
                rs_send[number, piece], unit = coded(part)
                cv_send[number, piece] = to_row([column, unit])
            for offset, piece in zip(offsets, pieces):
                line = cv_send.at[number, piece]
                codes = rs_send.at[number, piece]
                if offset == ENDS[0]:
                    for place, end in enumerate(ENDS):
                        band = pl.ds(place * top, top)
                        send(line, cv_recv.at[number, 6 + place], 1, number, chip(end))
                        send(
                            codes.at[band], rs_recv.at[number, 6, band], 0, number, chip(end)
                        )
                elif offset:
                    slot_id = FULL.index(offset)
                    send(line, cv_recv.at[number, slot_id], 1, number, chip(offset))
                    send(codes, rs_recv.at[number, slot_id], 0, number, chip(offset))
        meanwhile()
        arrived(cv_recv.at[number], 1, number)
        sums = to_row([column])
        for slot_id in range(7):
            sums += cv_recv[number, slot_id]
        sums = to_column(sums, 0)
        upper = lax.broadcasted_iota(jnp.int32, (traits, 1), 0) < top
        arrived(rs_recv.at[number], 0, number)
        total = rs_own[...]
        for slot_id in range(6):
            total += decoded(rs_recv[number, slot_id], to_column(cv_recv[number, slot_id], 1))
        unit = jnp.where(upper, to_column(cv_recv[number, 6], 1), to_column(cv_recv[number, 7], 1))
        total += decoded(rs_recv[number, 6], unit)
        mid[number, g], unit = coded(total)
        mcv[number, g] = to_row([sums, unit])

        def pass_on(group, offset, stage):
            send(mcv.at[number, group], mcv.at[number, group], stage + 1, number, chip(offset))
            send(mid.at[number, group], mid.at[number, group], stage, number, chip(offset))

        if not relay:
            pass_on(g, 2 * NEAR, 10)
        pass_on(g, NEAR, 2)
        pass_on(g, -NEAR, 8)
        arrived(mcv.at[number, 0], 9, number)
        arrived(mid.at[number, 0], 8, number)
        if relay:
            pass_on(lax.rem(g + 1, groups), -NEAR, 10)
        arrived(mcv.at[number, 0], 3, number)
        arrived(mid.at[number, 0], 2, number)
        arrived(mcv.at[number, 0], 11, number)
        arrived(mid.at[number, 0], 10, number)
        sums = mcv[number, 0]
        total = decoded(mid[number, 0], to_column(sums, 1))
        for group in range(1, groups):
            line = mcv[number, group]
            sums += line
            total += decoded(mid[number, group], to_column(line, 1))
        return total, to_column(sums, 0)

    def share(number, search, step):
        ag[number, r] = search.astype(BF16)
        for place, end in enumerate(ENDS):
            band = pl.ds(place * top, top)
            send(ag.at[number, r, band], ag.at[number, r, band], TAKE_OF[end], number, chip(end))
        agn[number, r] = to_row([jnp.sum(search * search, axis=1, keepdims=True), step])
        send(agn.at[number, r], agn.at[number, r], 5, number, chip(ENDS[0]))
        for offset in FULL:
            send(ag.at[number, r], ag.at[number, r], TAKE_OF[offset], number, chip(offset))
            send(agn.at[number, r], agn.at[number, r], 5, number, chip(offset))

    def image_of(number, fresh):
        own = jnp.zeros((traits, rows), F32)
        pair = jnp.zeros((traits, rows), F32)
        squares = jnp.zeros((traits, 1), F32)
        cross = jnp.zeros((traits, 1), F32)
        for stage, offsets in enumerate(TAKES):
            arrived(ag.at[number, pl.ds(0, len(offsets) - (0 in offsets))], 12 + stage, number)
            for offset in offsets:
                piece = piece_at(offset)
                low = ag[number, piece]
                own += lax.dot_general(low, xh[0, piece], NT, preferred_element_type=F32)
                pair += lax.dot_general(low, xh[1, piece], NT, preferred_element_type=F32)
                wide = low.astype(F32)
                squares += jnp.sum(wide * wide, axis=1, keepdims=True)
                if not fresh:
                    cross += jnp.sum(wide * dir_ref[piece], axis=1, keepdims=True)
        img_send[number, 0] = pair
        img_send[number, 1] = own
        send(img_send.at[number], img_recv.at[number], 6, number, partner)
        arrived(agn.at[number, pl.ds(0, NEAR - 1)], 5, number)
        line = agn[number, 0]
        for place in range(1, NEAR):
            line += agn[number, place]
        dd_send[number] = to_row([to_column(line, 0), squares, cross])
        send(dd_send.at[number], dd_recv.at[number], 7, number, partner)
        step = to_column(agn[number, 0], 1)
        if not fresh:
            fitted[...] += step[None] * img[...]
            acc[...] += step[None] * dir_ref[...]
        arrived(dd_recv.at[number], 7, number)
        line = dd_send[number] + dd_recv[number]
        norm = to_column(line, 0)
        squares = to_column(line, 1)
        arrived(img_recv.at[number], 6, number)
        own = mask_own * (own + img_recv[number, 0])
        pair = mask_pair * (pair + img_recv[number, 1])
        if fresh:
            ratio = jnp.zeros((traits, 1), F32)
        else:
            ratio = norm / vals[3][:, 0:1]
            own += ratio * img[0]
            pair += ratio * img[1]
            squares += ratio * (2.0 * to_column(line, 2) + ratio * vals[5][:, 0:1])
        img[0] = own
        img[1] = pair
        vals[3] = jnp.broadcast_to(norm, (traits, 128))
        vals[4] = jnp.broadcast_to(step, (traits, 128))
        vals[5] = jnp.broadcast_to(squares, (traits, 128))
        vals[6] = jnp.broadcast_to(ratio, (traits, 128))

    def turn(number):
        dir_ref[...] = ag[number].astype(F32) + vals[6][:, 0:1][None] * dir_ref[...]

    zero = jnp.zeros((traits, 1), F32)
    total, _ = sum_for_owner(0, lambda piece: dir_ref[piece] + drecv[piece], zero, True)
    search = total / noise_var + jnp.sqrt(ridge) * nco[...]
    search_ref[...] = search
    share(0, search, zero)
    swap_res.wait_recv()
    swap_geno.wait_recv()
    image_of(0, True)
    dir_ref[...] = jnp.zeros_like(dir_ref)

    def iterate(number, carry):
        own, pair = img[0], img[1]
        own_low = own.astype(BF16)
        pair_low = pair.astype(BF16)
        bend = jnp.sum(own * own_low.astype(F32), axis=1, keepdims=True)
        bend += jnp.sum(pair * pair_low.astype(F32), axis=1, keepdims=True)

        def part_of(piece):
            part = lax.dot_general(own_low, xh[0, piece], NN, preferred_element_type=F32)
            return part + lax.dot_general(pair_low, xh[1, piece], NN, preferred_element_type=F32)

        def meanwhile():
            turn(number - 1)

        total, bend = sum_for_owner(number, part_of, bend, False, meanwhile)
        step = vals[3][:, 0:1] / (bend / noise_var + ridge * vals[5][:, 0:1])
        applied = total / noise_var + ridge * dir_ref[r]
        search = search_ref[...] - step * applied
        search_ref[...] = search
        share(number, search, step)
        image_of(number, False)
        return carry

    lax.fori_loop(1, ITERS, iterate, 0)
    turn(ITERS - 1)

    swap_acc = to_pair(acc, c_recv, 3)
    swap_dir = to_pair(dir_ref, d_recv, 4)
    own, pair = img[0], img[1]
    squares = vals[5][:, 0:1]
    guess = vals[4][:, 0:1]
    left_own = pres[0] - fitted[0] - guess * own
    left_pair = pres[1] - fitted[1] - guess * pair

    def both(one, two):
        return jnp.sum(one, axis=1, keepdims=True) + jnp.sum(two, axis=1, keepdims=True)

    fin[z] = to_row(
        [
            both(own * own.astype(BF16).astype(F32), pair * pair.astype(BF16).astype(F32)),
            both(left_own * left_own, left_pair * left_pair),
            both(left_own * own, left_pair * pair),
            both(own * own, pair * pair),
        ]
    )
    half_way = chips // 2
    for offset in sorted(range(1, chips), key=lambda o: -min(o, chips - o)):
        pltpu.make_async_remote_copy(
            src_ref=fin.at[z],
            dst_ref=fin.at[z],
            send_sem=pair_send.at[5],
            recv_sem=pair_recv.at[5],
            device_id=chip(offset if offset <= half_way else offset - chips),
            device_id_type=MESH,
        ).start()
    swap_acc.start()
    swap_dir.start()
    present = jnp.int32(0)
    for device in range(chips * CORES):
        present += s_counts[device]
    others = fin.at[pl.ds(0, chips - 1)]
    pltpu.make_async_copy(others, others, pair_recv.at[5]).wait()
    line = fin[0]
    for place in range(1, chips):
        line += fin[place]
    norm_now = vals[3][:, 0:1]
    step = norm_now / (to_column(line, 0) / noise_var + ridge * squares)
    shift = step - guess
    left = to_column(line, 1) - 2.0 * shift * to_column(line, 2) + shift * shift * to_column(line, 3)
    scale = (present.astype(F32) + PRIOR_DOF) * vals[2][:, 0:1]
    sigma_out[...] = to_row([(left + PRIOR_DOF * PRIOR_SCALE) / scale])
    resid_out[...] = pres[0] - (fitted[0] + step * own)

    def put(start, place, steps, directions):
        for piece in range(NEAR):
            columns = slice(piece * width, (piece + 1) * width)
            new = steps[piece] + step * directions[piece]
            at = pl.multiple_of(start + piece * width, width)
            coef_out[:, pl.ds(at, width)] = jnp.where(first, new, cf[place, :, columns])
            at = pl.multiple_of(CORES * half + start + piece * width, width)
            coef_out[:, pl.ds(at, width)] = jnp.where(first, cf[place + 2, :, columns], new)

    put(mine, 0, acc, dir_ref)
    swap_acc.wait_recv()
    swap_dir.wait_recv()
    put(other, 1, c_recv, d_recv)

    for swap in (swap_sum, swap_res, swap_geno, swap_acc, swap_dir):
        swap.wait_send()
    pltpu.make_async_copy(others, others, pair_send.at[5]).wait()

    def sent(ref, stage, number):
        pltpu.make_async_copy(ref, ref, st_send.at[number, stage]).wait()

    def drain(number, carry):
        sent(rs_recv.at[number], 0, number)
        sent(cv_recv.at[number], 1, number)
        for stage in (2, 8, 10):
            sent(mid.at[number, 0], stage, number)
            sent(mcv.at[number, 0], stage + 1, number)
        sent(agn.at[number, pl.ds(0, NEAR - 1)], 5, number)
        sent(img_recv.at[number], 6, number)
        sent(dd_recv.at[number], 7, number)
        for stage, offsets in enumerate(TAKES):
            sent(ag.at[number, pl.ds(0, len(offsets) - (0 in offsets))], 12 + stage, number)
        return carry

    lax.fori_loop(0, ITERS, drain, 0)


def loose(array):
    return pltpu.with_memory_space_constraint(array, pltpu.HBM)


def update(geno, resid, npeople, ncoef, coef, block, prior, sigma, gamma, counts):
    rows, batch = geno.shape
    traits = resid.shape[0]
    devices = lax.axis_size(AXIS)
    chips = devices // CORES
    half = batch // CORES
    width = half // NEAR
    groups = chips // NEAR
    outside = pl.BlockSpec(memory_space=pltpu.HBM)
    inside = pl.BlockSpec(memory_space=pltpu.VMEM)
    block16 = (NEAR, traits, width)
    return pl.pallas_call(
        functools.partial(kernel, chips),
        name="gibbs",
        out_shape=(
            jax.ShapeDtypeStruct(coef.shape, F32),
            jax.ShapeDtypeStruct((traits, rows), F32),
            jax.ShapeDtypeStruct((1, 128), F32),
        ),
        in_specs=[outside] * 10,
        out_specs=(inside,) * 3,
        scratch_shapes=[
            pltpu.VMEM((2, NEAR, rows, width), BF16),
            pltpu.VMEM((NEAR, rows, width), BF16),
            pltpu.VMEM((4, traits, half), F32),
            pltpu.VMEM((traits, rows), F32),
            pltpu.VMEM((traits, rows), F32),
            pltpu.VMEM((traits, width), F32),
            pltpu.SMEM((1,), jnp.int32),
            pltpu.SMEM((traits,), F32),
            pltpu.SMEM((traits,), F32),
            pltpu.SMEM((traits,), F32),
            pltpu.SMEM((devices,), jnp.int32),
            pltpu.VMEM((2, traits, rows), F32),
            pltpu.VMEM(block16, F32),
            pltpu.VMEM(block16, F32),
            pltpu.VMEM((traits, width), F32),
            pltpu.VMEM((ITERS, *block16), jnp.int16),
            pltpu.VMEM((ITERS, 7, traits, width), jnp.int16),
            pltpu.VMEM((ITERS, NEAR, 1, 128), F32),
            pltpu.VMEM((ITERS, 8, 1, 128), F32),
            pltpu.VMEM((ITERS, groups, traits, width), jnp.int16),
            pltpu.VMEM((ITERS, groups, 1, 128), F32),
            pltpu.VMEM((ITERS, *block16), BF16),
            pltpu.VMEM((ITERS, NEAR, 1, 128), F32),
            pltpu.VMEM((traits, width), F32),
            pltpu.VMEM(block16, F32),
            pltpu.VMEM(block16, F32),
            pltpu.VMEM((ITERS, 2, traits, rows), F32),
            pltpu.VMEM((ITERS, 2, traits, rows), F32),
            pltpu.VMEM((ITERS, 1, 128), F32),
            pltpu.VMEM((ITERS, 1, 128), F32),
            pltpu.VMEM((2, traits, rows), F32),
            pltpu.VMEM((2, traits, rows), F32),
            pltpu.VMEM((chips, 1, 128), F32),
            pltpu.VMEM(block16, F32),
            pltpu.VMEM(block16, F32),
            pltpu.VMEM((7, traits, 128), F32),
            pltpu.SemaphoreType.DMA((23,)),
            pltpu.SemaphoreType.DMA((5,)),
            pltpu.SemaphoreType.DMA((6,)),
            pltpu.SemaphoreType.DMA((6,)),
            pltpu.SemaphoreType.DMA((ITERS, 15)),
            pltpu.SemaphoreType.DMA((ITERS, 15)),
        ],
        compiler_params=pltpu.CompilerParams(
            collective_id=0, has_side_effects=True, vmem_limit_bytes=40 * 1000 * 1000


        ),
    )(
        *map(loose, (geno, resid, npeople, ncoef, coef)),
        block,
        *map(loose, (prior, sigma, gamma, counts)),
    )


def per_device(geno, resid, npeople, ncoef, coef, block, prior, sigma, gamma, counts):
    coef_new, resid_new, sigma_line = update(
        geno, resid, npeople, ncoef, coef, block, prior, sigma, gamma, counts
    )
    return coef_new, resid_new, sigma_line[0, : resid.shape[0]]


def solution(mesh):
    return jax.shard_map(
        per_device,
        mesh=mesh,
        in_specs=(
            P(("trait", "ppl"), None),
            P("trait", "ppl"),
            P("trait", "ppl"),
            P("trait", None),
            P("trait", None),
            P("trait"),
            P("trait"),
            P("trait"),
            P("trait"),
            P("trait"),
        ),
        out_specs=(P("trait", None), P("trait", "ppl"), P("trait")),
        check_vma=False,
    )
```

```python
import functools

import jax
import jax.numpy as jnp
from jax import lax
from jax.experimental import pallas as pl
from jax.experimental.pallas import tpu as pltpu
from jax.sharding import PartitionSpec as P

ITERS = 4
PRIOR_DOF = 4.0
PRIOR_SCALE = 0.5
AXIS = "ppl"
CORES = 2
NEAR = 8
MESH = pl.DeviceIdType.MESH
F32 = jnp.float32
BF16 = jnp.bfloat16
NT = (((1,), (1,)), ((), ()))
NN = (((1,), (0,)), ((), ()))
CODES = 32000.0
FULL = (3, -3, 2, -2, 1, -1)
ENDS = (NEAR // 2, -(NEAR // 2))
SENDS = ((NEAR // 2, 3, -3), (2, -2), (1, -1), (0,))
TAKES = ((0, 1, -1), (2, -2), (3, -3, NEAR // 2))
TAKE_OF = {sign * abs(o): 12 + i for i, offsets in enumerate(TAKES) for o in offsets for sign in (1, -1)}


def kernel(
    chips,
    geno,
    resid,
    npeople,
    ncoef,
    coef,
    block,
    prior,
    sigma,
    gamma,
    counts,
    coef_out,
    resid_out,
    sigma_out,
    xh,
    xo,
    cf,
    res,
    npl,
    nco,
    s_block,
    s_prior,
    s_sigma,
    s_gamma,
    s_counts,
    pres,
    dsend,
    drecv,
    rs_own,
    rs_send,
    rs_recv,
    cv_send,
    cv_recv,
    mid,
    mcv,
    ag,
    agn,
    search_ref,
    dir_ref,
    acc,
    img_send,
    img_recv,
    dd_send,
    dd_recv,
    img,
    fitted,
    fin,
    c_recv,
    d_recv,
    vals,
    load_sem,
    small_sem,
    pair_send,
    pair_recv,
    st_send,
    st_recv,
):
    traits, rows = res.shape
    width = xo.shape[2]
    half = NEAR * width
    groups = chips // NEAR
    top = traits // 2
    me = lax.axis_index(AXIS)
    z = me // CORES
    k = lax.rem(me, CORES)
    g = z // NEAR
    r = lax.rem(z, NEAR)
    partner = {AXIS: z * CORES + (1 - k)}

    near = {o: {AXIS: lax.rem(z + o + chips, chips) * CORES + k} for o in (*ENDS, *FULL, NEAR, -NEAR)}

    def chip(offset):
        return near.get(offset) or {AXIS: lax.rem(z + offset + chips, chips) * CORES + k}

    def piece_at(offset):
        return lax.rem(r + offset + NEAR, NEAR)

    mine = pl.multiple_of(k * half, half)
    other = pl.multiple_of((1 - k) * half, half)
    own_col = pl.multiple_of(k * half + r * width, width)
    loads = [
        pltpu.make_async_copy(coef.at[:, pl.ds(mine, half)], cf.at[0], load_sem.at[0]),
        pltpu.make_async_copy(coef.at[:, pl.ds(other, half)], cf.at[1], load_sem.at[1]),
        pltpu.make_async_copy(coef.at[:, pl.ds(2 * half + mine, half)], cf.at[2], load_sem.at[2]),
        pltpu.make_async_copy(coef.at[:, pl.ds(2 * half + other, half)], cf.at[3], load_sem.at[3]),
        pltpu.make_async_copy(resid, res, load_sem.at[4]),
        pltpu.make_async_copy(npeople, npl, load_sem.at[5]),
        pltpu.make_async_copy(ncoef.at[:, pl.ds(own_col, width)], nco, load_sem.at[6]),
    ]
    for piece in range(NEAR):
        at = pl.multiple_of(mine + piece * width, width)
        loads.append(
            pltpu.make_async_copy(geno.at[:, pl.ds(at, width)], xh.at[0, piece], load_sem.at[7 + piece])
        )
        at = pl.multiple_of(other + piece * width, width)
        loads.append(
            pltpu.make_async_copy(geno.at[:, pl.ds(at, width)], xo.at[piece], load_sem.at[15 + piece])
        )
    smalls = [
        pltpu.make_async_copy(block, s_block, small_sem.at[0]),
        pltpu.make_async_copy(prior, s_prior, small_sem.at[1]),
        pltpu.make_async_copy(sigma, s_sigma, small_sem.at[2]),
        pltpu.make_async_copy(gamma, s_gamma, small_sem.at[3]),
        pltpu.make_async_copy(counts, s_counts, small_sem.at[4]),
    ]
    for copy in smalls + loads:
        copy.start()
    barrier = pltpu.get_barrier_semaphore()
    for target in (*[chip(offset) for offset in (*ENDS, *FULL)], partner):
        pl.semaphore_signal(barrier, inc=1, device_id=target, device_id_type=MESH)
    for copy in smalls:
        copy.wait()

    row_id = lax.broadcasted_iota(jnp.int32, (traits, 128), 0)
    lane_id = lax.broadcasted_iota(jnp.int32, (traits, 128), 1)

    def to_row(columns):
        total = jnp.zeros((traits, 128), F32)
        for place, column in enumerate(columns):
            total += jnp.where(lane_id == row_id + place * traits, column, 0.0)
        return jnp.sum(total, axis=0, keepdims=True)

    def to_column(line, place):
        return jnp.sum(
            jnp.where(lane_id == row_id + place * traits, line, 0.0), axis=1, keepdims=True
        )

    def column_of(ref):
        column = jnp.zeros((traits, 128), F32)
        for trait in range(traits):
            column = jnp.where(row_id == trait, ref[trait], column)
        return column

    vals[0] = column_of(s_sigma)
    vals[1] = column_of(s_prior)
    vals[2] = column_of(s_gamma)
    noise_var = vals[0][:, 0:1]
    ridge = vals[1][:, 0:1]
    slot = lax.broadcasted_iota(jnp.int32, (traits, rows), 1)
    mask_own = (slot < s_counts[me]).astype(F32)
    mask_pair = (slot < s_counts[z * CORES + (1 - k)]).astype(F32)

    def coded(values):
        largest = jnp.maximum(jnp.max(jnp.abs(values), axis=1, keepdims=True), 1e-30)
        codes = jnp.round(values * (CODES / largest)).astype(jnp.int32).astype(jnp.int16)
        return codes, largest * (1.0 / CODES)

    def decoded(codes, unit):
        return codes.astype(jnp.int32).astype(F32) * unit

    for copy in loads:
        copy.wait()
    first = s_block[0] == 0
    old_mine = jnp.where(first, cf[0], cf[2]).astype(BF16)
    old_other = jnp.where(first, cf[1], cf[3]).astype(BF16)
    fitted_old = jnp.zeros((traits, rows), F32)
    for piece in range(NEAR):
        columns = slice(piece * width, (piece + 1) * width)
        fitted_old += lax.dot_general(old_mine[:, columns], xh[0, piece], NT, preferred_element_type=F32)
        fitted_old += lax.dot_general(old_other[:, columns], xo[piece], NT, preferred_element_type=F32)
    partial_res = mask_own * (res[...] + fitted_old)
    pres[0] = partial_res
    target = (mask_own * (partial_res + jnp.sqrt(noise_var) * npl[...])).astype(BF16)
    for piece in range(NEAR):
        dsend[piece] = lax.dot_general(target, xo[piece], NN, preferred_element_type=F32)

    pl.semaphore_wait(barrier, len(ENDS) + len(FULL) + 1)

    def to_pair(src, dst, index):
        return pltpu.make_async_remote_copy(
            src_ref=src,
            dst_ref=dst,
            send_sem=pair_send.at[index],
            recv_sem=pair_recv.at[index],
            device_id=partner,
            device_id_type=MESH,
        )

    swap_sum = to_pair(dsend, drecv, 0)
    swap_res = to_pair(pres.at[0], pres.at[1], 1)
    swap_geno = to_pair(xo, xh.at[1], 2)
    swap_sum.start()
    swap_res.start()
    for piece in range(NEAR):
        dir_ref[piece] = lax.dot_general(target, xh[0, piece], NN, preferred_element_type=F32)
    fitted[...] = jnp.zeros_like(fitted)
    acc[...] = jnp.zeros_like(acc)
    swap_sum.wait_recv()

    def send(src, dst, stage, number, target):
        pltpu.make_async_remote_copy(
            src_ref=src,
            dst_ref=dst,
            send_sem=st_send.at[number, stage],
            recv_sem=st_recv.at[number, stage],
            device_id=target,
            device_id_type=MESH,
        ).start()

    def arrived(ref, stage, number):
        pltpu.make_async_copy(ref, ref, st_recv.at[number, stage]).wait()

    def sum_for_owner(number, part_of, column, relay, meanwhile):
        for offsets in SENDS:
            pieces = [piece_at(offset) for offset in offsets]
            for offset, piece, part in zip(offsets, pieces, [part_of(piece) for piece in pieces]):
                if offset == 0:
                    rs_own[...] = part
                    continue
                rs_send[number, piece], unit = coded(part)
                cv_send[number, piece] = to_row([column, unit])
            for offset, piece in zip(offsets, pieces):
                line = cv_send.at[number, piece]
                codes = rs_send.at[number, piece]
                if offset == ENDS[0]:
                    for place, end in enumerate(ENDS):
                        band = pl.ds(place * top, top)
                        send(line, cv_recv.at[number, 6 + place], 1, number, chip(end))
                        send(
                            codes.at[band], rs_recv.at[number, 6, band], 0, number, chip(end)
                        )
                elif offset:
                    slot_id = FULL.index(offset)
                    send(line, cv_recv.at[number, slot_id], 1, number, chip(offset))
                    send(codes, rs_recv.at[number, slot_id], 0, number, chip(offset))
        arrived(cv_recv.at[number], 1, number)
        sums = to_row([column])
        for slot_id in range(7):
            sums += cv_recv[number, slot_id]
        sums = to_column(sums, 0)
        upper = lax.broadcasted_iota(jnp.int32, (traits, 1), 0) < top
        arrived(rs_recv.at[number], 0, number)
        total = rs_own[...]
        for slot_id in range(6):
            total += decoded(rs_recv[number, slot_id], to_column(cv_recv[number, slot_id], 1))
        unit = jnp.where(upper, to_column(cv_recv[number, 6], 1), to_column(cv_recv[number, 7], 1))
        total += decoded(rs_recv[number, 6], unit)
        mid[number, g], unit = coded(total)
        mcv[number, g] = to_row([sums, unit])

        def pass_on(group, offset, stage):
            send(mcv.at[number, group], mcv.at[number, group], stage + 1, number, chip(offset))
            send(mid.at[number, group], mid.at[number, group], stage, number, chip(offset))

        if not relay:
            pass_on(g, 2 * NEAR, 10)
        pass_on(g, NEAR, 2)
        pass_on(g, -NEAR, 8)
        meanwhile()
        arrived(mcv.at[number, 0], 9, number)
        arrived(mid.at[number, 0], 8, number)
        if relay:
            pass_on(lax.rem(g + 1, groups), -NEAR, 10)
        arrived(mcv.at[number, 0], 3, number)
        arrived(mid.at[number, 0], 2, number)
        arrived(mcv.at[number, 0], 11, number)
        arrived(mid.at[number, 0], 10, number)
        sums = mcv[number, 0]
        total = decoded(mid[number, 0], to_column(sums, 1))
        for group in range(1, groups):
            line = mcv[number, group]
            sums += line
            total += decoded(mid[number, group], to_column(line, 1))
        return total, to_column(sums, 0)

    def share(number, search, step):
        ag[number, r] = search.astype(BF16)
        for place, end in enumerate(ENDS):
            band = pl.ds(place * top, top)
            send(ag.at[number, r, band], ag.at[number, r, band], TAKE_OF[end], number, chip(end))
        agn[number, r] = to_row([jnp.sum(search * search, axis=1, keepdims=True), step])
        send(agn.at[number, r], agn.at[number, r], 5, number, chip(ENDS[0]))
        for offset in FULL:
            send(ag.at[number, r], ag.at[number, r], TAKE_OF[offset], number, chip(offset))
            send(agn.at[number, r], agn.at[number, r], 5, number, chip(offset))

    def image_of(number, fresh):
        own = jnp.zeros((traits, rows), F32)
        pair = jnp.zeros((traits, rows), F32)
        squares = jnp.zeros((traits, 1), F32)
        cross = jnp.zeros((traits, 1), F32)
        for stage, offsets in enumerate(TAKES):
            arrived(ag.at[number, pl.ds(0, len(offsets) - (0 in offsets))], 12 + stage, number)
            for offset in offsets:
                piece = piece_at(offset)
                low = ag[number, piece]
                own += lax.dot_general(low, xh[0, piece], NT, preferred_element_type=F32)
                pair += lax.dot_general(low, xh[1, piece], NT, preferred_element_type=F32)
                wide = low.astype(F32)
                squares += jnp.sum(wide * wide, axis=1, keepdims=True)
                if not fresh:
                    cross += jnp.sum(wide * dir_ref[piece], axis=1, keepdims=True)
        img_send[number, 0] = pair
        img_send[number, 1] = own
        send(img_send.at[number], img_recv.at[number], 6, number, partner)
        arrived(agn.at[number, pl.ds(0, NEAR - 1)], 5, number)
        line = agn[number, 0]
        for place in range(1, NEAR):
            line += agn[number, place]
        dd_send[number] = to_row([to_column(line, 0), squares, cross])
        send(dd_send.at[number], dd_recv.at[number], 7, number, partner)
        step = to_column(agn[number, 0], 1)
        if not fresh:
            fitted[...] += step[None] * img[...]
            acc[...] += step[None] * dir_ref[...]
        arrived(dd_recv.at[number], 7, number)
        line = dd_send[number] + dd_recv[number]
        norm = to_column(line, 0)
        squares = to_column(line, 1)
        arrived(img_recv.at[number], 6, number)
        own = mask_own * (own + img_recv[number, 0])
        pair = mask_pair * (pair + img_recv[number, 1])
        if fresh:
            ratio = jnp.zeros((traits, 1), F32)
        else:
            ratio = norm / vals[3][:, 0:1]
            own += ratio * img[0]
            pair += ratio * img[1]
            squares += ratio * (2.0 * to_column(line, 2) + ratio * vals[5][:, 0:1])
        img[0] = own
        img[1] = pair
        vals[3] = jnp.broadcast_to(norm, (traits, 128))
        vals[4] = jnp.broadcast_to(step, (traits, 128))
        vals[5] = jnp.broadcast_to(squares, (traits, 128))
        vals[6] = jnp.broadcast_to(ratio, (traits, 128))

    def turn(number):
        dir_ref[...] = ag[number].astype(F32) + vals[6][:, 0:1][None] * dir_ref[...]

    zero = jnp.zeros((traits, 1), F32)
    total, _ = sum_for_owner(0, lambda piece: dir_ref[piece] + drecv[piece], zero, True, swap_geno.start)
    search = total / noise_var + jnp.sqrt(ridge) * nco[...]
    search_ref[...] = search
    share(0, search, zero)
    swap_res.wait_recv()
    swap_geno.wait_recv()
    image_of(0, True)
    dir_ref[...] = jnp.zeros_like(dir_ref)

    def iterate(number, carry):
        own, pair = img[0], img[1]
        own_low = own.astype(BF16)
        pair_low = pair.astype(BF16)
        bend = jnp.sum(own * own_low.astype(F32), axis=1, keepdims=True)
        bend += jnp.sum(pair * pair_low.astype(F32), axis=1, keepdims=True)

        def part_of(piece):
            part = lax.dot_general(own_low, xh[0, piece], NN, preferred_element_type=F32)
            return part + lax.dot_general(pair_low, xh[1, piece], NN, preferred_element_type=F32)

        def meanwhile():
            turn(number - 1)

        total, bend = sum_for_owner(number, part_of, bend, False, meanwhile)
        step = vals[3][:, 0:1] / (bend / noise_var + ridge * vals[5][:, 0:1])
        applied = total / noise_var + ridge * dir_ref[r]
        search = search_ref[...] - step * applied
        search_ref[...] = search
        share(number, search, step)
        image_of(number, False)
        return carry

    lax.fori_loop(1, ITERS, iterate, 0)
    turn(ITERS - 1)

    swap_acc = to_pair(acc, c_recv, 3)
    swap_dir = to_pair(dir_ref, d_recv, 4)
    own, pair = img[0], img[1]
    squares = vals[5][:, 0:1]
    guess = vals[4][:, 0:1]
    left_own = pres[0] - fitted[0] - guess * own
    left_pair = pres[1] - fitted[1] - guess * pair

    def both(one, two):
        return jnp.sum(one, axis=1, keepdims=True) + jnp.sum(two, axis=1, keepdims=True)

    fin[z] = to_row(
        [
            both(own * own.astype(BF16).astype(F32), pair * pair.astype(BF16).astype(F32)),
            both(left_own * left_own, left_pair * left_pair),
            both(left_own * own, left_pair * pair),
            both(own * own, pair * pair),
        ]
    )
    half_way = chips // 2
    for offset in sorted(range(1, chips), key=lambda o: -min(o, chips - o)):
        pltpu.make_async_remote_copy(
            src_ref=fin.at[z],
            dst_ref=fin.at[z],
            send_sem=pair_send.at[5],
            recv_sem=pair_recv.at[5],
            device_id=chip(offset if offset <= half_way else offset - chips),
            device_id_type=MESH,
        ).start()
    swap_acc.start()
    swap_dir.start()
    present = jnp.int32(0)
    for device in range(chips * CORES):
        present += s_counts[device]
    others = fin.at[pl.ds(0, chips - 1)]
    pltpu.make_async_copy(others, others, pair_recv.at[5]).wait()
    line = fin[0]
    for place in range(1, chips):
        line += fin[place]
    norm_now = vals[3][:, 0:1]
    step = norm_now / (to_column(line, 0) / noise_var + ridge * squares)
    shift = step - guess
    left = to_column(line, 1) - 2.0 * shift * to_column(line, 2) + shift * shift * to_column(line, 3)
    scale = (present.astype(F32) + PRIOR_DOF) * vals[2][:, 0:1]
    sigma_out[...] = to_row([(left + PRIOR_DOF * PRIOR_SCALE) / scale])
    resid_out[...] = pres[0] - (fitted[0] + step * own)

    def put(start, place, steps, directions):
        for piece in range(NEAR):
            columns = slice(piece * width, (piece + 1) * width)
            new = steps[piece] + step * directions[piece]
            at = pl.multiple_of(start + piece * width, width)
            coef_out[:, pl.ds(at, width)] = jnp.where(first, new, cf[place, :, columns])
            at = pl.multiple_of(CORES * half + start + piece * width, width)
            coef_out[:, pl.ds(at, width)] = jnp.where(first, cf[place + 2, :, columns], new)

    put(mine, 0, acc, dir_ref)
    swap_acc.wait_recv()
    swap_dir.wait_recv()
    put(other, 1, c_recv, d_recv)

    for swap in (swap_sum, swap_res, swap_geno, swap_acc, swap_dir):
        swap.wait_send()
    pltpu.make_async_copy(others, others, pair_send.at[5]).wait()

    def sent(ref, stage, number):
        pltpu.make_async_copy(ref, ref, st_send.at[number, stage]).wait()

    def drain(number, carry):
        sent(rs_recv.at[number], 0, number)
        sent(cv_recv.at[number], 1, number)
        for stage in (2, 8, 10):
            sent(mid.at[number, 0], stage, number)
            sent(mcv.at[number, 0], stage + 1, number)
        sent(agn.at[number, pl.ds(0, NEAR - 1)], 5, number)
        sent(img_recv.at[number], 6, number)
        sent(dd_recv.at[number], 7, number)
        for stage, offsets in enumerate(TAKES):
            sent(ag.at[number, pl.ds(0, len(offsets) - (0 in offsets))], 12 + stage, number)
        return carry

    lax.fori_loop(0, ITERS, drain, 0)


def loose(array):
    return pltpu.with_memory_space_constraint(array, pltpu.HBM)


def update(geno, resid, npeople, ncoef, coef, block, prior, sigma, gamma, counts):
    rows, batch = geno.shape
    traits = resid.shape[0]
    devices = lax.axis_size(AXIS)
    chips = devices // CORES
    half = batch // CORES
    width = half // NEAR
    groups = chips // NEAR
    outside = pl.BlockSpec(memory_space=pltpu.HBM)
    inside = pl.BlockSpec(memory_space=pltpu.VMEM)
    block16 = (NEAR, traits, width)
    return pl.pallas_call(
        functools.partial(kernel, chips),
        name="gibbs",
        out_shape=(
            jax.ShapeDtypeStruct(coef.shape, F32),
            jax.ShapeDtypeStruct((traits, rows), F32),
            jax.ShapeDtypeStruct((1, 128), F32),
        ),
        in_specs=[outside] * 10,
        out_specs=(inside,) * 3,
        scratch_shapes=[
            pltpu.VMEM((2, NEAR, rows, width), BF16),
            pltpu.VMEM((NEAR, rows, width), BF16),
            pltpu.VMEM((4, traits, half), F32),
            pltpu.VMEM((traits, rows), F32),
            pltpu.VMEM((traits, rows), F32),
            pltpu.VMEM((traits, width), F32),
            pltpu.SMEM((1,), jnp.int32),
            pltpu.SMEM((traits,), F32),
            pltpu.SMEM((traits,), F32),
            pltpu.SMEM((traits,), F32),
            pltpu.SMEM((devices,), jnp.int32),
            pltpu.VMEM((2, traits, rows), F32),
            pltpu.VMEM(block16, F32),
            pltpu.VMEM(block16, F32),
            pltpu.VMEM((traits, width), F32),
            pltpu.VMEM((ITERS, *block16), jnp.int16),
            pltpu.VMEM((ITERS, 7, traits, width), jnp.int16),
            pltpu.VMEM((ITERS, NEAR, 1, 128), F32),
            pltpu.VMEM((ITERS, 8, 1, 128), F32),
            pltpu.VMEM((ITERS, groups, traits, width), jnp.int16),
            pltpu.VMEM((ITERS, groups, 1, 128), F32),
            pltpu.VMEM((ITERS, *block16), BF16),
            pltpu.VMEM((ITERS, NEAR, 1, 128), F32),
            pltpu.VMEM((traits, width), F32),
            pltpu.VMEM(block16, F32),
            pltpu.VMEM(block16, F32),
            pltpu.VMEM((ITERS, 2, traits, rows), F32),
            pltpu.VMEM((ITERS, 2, traits, rows), F32),
            pltpu.VMEM((ITERS, 1, 128), F32),
            pltpu.VMEM((ITERS, 1, 128), F32),
            pltpu.VMEM((2, traits, rows), F32),
            pltpu.VMEM((2, traits, rows), F32),
            pltpu.VMEM((chips, 1, 128), F32),
            pltpu.VMEM(block16, F32),
            pltpu.VMEM(block16, F32),
            pltpu.VMEM((7, traits, 128), F32),
            pltpu.SemaphoreType.DMA((23,)),
            pltpu.SemaphoreType.DMA((5,)),
            pltpu.SemaphoreType.DMA((6,)),
            pltpu.SemaphoreType.DMA((6,)),
            pltpu.SemaphoreType.DMA((ITERS, 15)),
            pltpu.SemaphoreType.DMA((ITERS, 15)),
        ],
        compiler_params=pltpu.CompilerParams(
            collective_id=0, has_side_effects=True, vmem_limit_bytes=40 * 1000 * 1000


        ),
    )(
        *map(loose, (geno, resid, npeople, ncoef, coef)),
        block,
        *map(loose, (prior, sigma, gamma, counts)),
    )


def per_device(geno, resid, npeople, ncoef, coef, block, prior, sigma, gamma, counts):
    coef_new, resid_new, sigma_line = update(
        geno, resid, npeople, ncoef, coef, block, prior, sigma, gamma, counts
    )
    return coef_new, resid_new, sigma_line[0, : resid.shape[0]]


def solution(mesh):
    return jax.shard_map(
        per_device,
        mesh=mesh,
        in_specs=(
            P(("trait", "ppl"), None),
            P("trait", "ppl"),
            P("trait", "ppl"),
            P("trait", None),
            P("trait", None),
            P("trait"),
            P("trait"),
            P("trait"),
            P("trait"),
            P("trait"),
        ),
        out_specs=(P("trait", None), P("trait", "ppl"), P("trait")),
        check_vma=False,
    )
```
